32 devices in a mesh: tok: 8 (over z, x), exp: 4 (over y, core).
Axes of the slice: x: 2, y: 2, z: 4, core: 2. Of those that a mesh axis runs over, the one named last changes fastest.
Arguments:
- tokens: bfloat16 [16384, 7168], P('tok', 'exp'), may hold values from -6 to 6
- gate_weight: bfloat16 [7168, 256], P('exp'), may hold values from -0.0625 to 0.0625
- expert_ids: int32 [16384, 8], P('tok'), may hold values from 0 to 255, all different within a row
- expert_bias: float32 [256], P('exp'), may hold values from -0.002 to 0.002
Outputs:
- affinities: float32 [16384, 256], P('tok', 'exp')
- weights: float32 [16384, 8], P('tok')
- load: float32 [256], replicated
- new_bias: float32 [256], replicated
The draws below stay inside these ranges and needn't reach their ends.
All inputs are finite; a program needn't handle non-finite values.
Results may differ from the reference program's by a relative error of at most 0.0003.
Values may be sent and summed in bfloat16 or wider, within the bound.
A program may use at most 64 MiB of HBM per device.

```python
import jax
import jax.numpy as jnp
from jax import lax

D = 7168
E = 256
TOPK = 8
TOKENS = 16384


def block_scale(rng, extent, shards, low, high):
    def one(axis_at, blocks):
        draws = jax.random.uniform(jax.random.fold_in(jax.random.fold_in(rng, 6), axis_at), (blocks,), jnp.float32, low / len(shards), high / len(shards))
        return jnp.repeat(jnp.exp(draws), extent[axis_at] // blocks).reshape((-1,) + (1,) * (len(extent) - axis_at - 1))

    loudness = one(*shards[0])
    for cut in shards[1:]:
        loudness = loudness * one(*cut)
    return loudness


def picks_of(stream_key, rows, count, top, lift):
    ranking = jax.random.permutation(jax.random.fold_in(stream_key, 1), count)
    boost = ranking
    for power in range(3):
        boost = boost * boost // count
    boost = boost * lift // count
    tickets = jax.random.randint(jax.random.fold_in(stream_key, 2), (rows, count), 0, 4096) + boost
    holders = jax.random.permutation(jax.random.fold_in(stream_key, 3), rows)[jnp.arange(count) % rows]
    tickets = jnp.where(jnp.arange(rows)[:, None] == holders[None, :], 1 << 14, tickets)
    priority = tickets * count + jnp.arange(count)
    return lax.top_k(priority.astype(jnp.int32), top)[1].astype(jnp.int32)


def gaussian(own_key, shape, deviation, bound, shards=(), kind=jnp.bfloat16):
    loudness = block_scale(own_key, shape, shards, -0.22, 0.18) if shards else 1.0
    values = jax.random.normal(own_key, shape, jnp.float32) * deviation * loudness
    return jnp.minimum(jnp.maximum(values, -bound), bound).astype(kind)


def setup_inputs(seed: int = 0) -> dict:
    key_of = jax.random.split(jax.random.key(seed), 5)
    tokens = gaussian(key_of[0], (TOKENS, D), 1.0, 6.0, ((0, 8), (1, 4)))
    gate_weight = gaussian(key_of[1], (D, E), D ** -0.5, 0.0625, ((0, 4),))
    expert_ids = picks_of(key_of[2], TOKENS, E, TOPK, 512)
    expert_bias = jnp.clip(jax.random.uniform(key_of[3], (E,), jnp.float32, -0.002, 0.002) * block_scale(key_of[3], (E,), ((0, 4),), -0.4, 0.0), -0.002, 0.002)
    return {"tokens": tokens, "gate_weight": gate_weight, "expert_ids": expert_ids, "expert_bias": expert_bias}


def reference(tokens, gate_weight, expert_ids, expert_bias):
    logits = jnp.dot(tokens, gate_weight, preferred_element_type=jnp.float32)
    affinities = jax.nn.sigmoid(logits)
    chosen = jnp.take_along_axis(affinities, expert_ids, axis=1)
    weights = 2.5 * chosen / jnp.sum(chosen, axis=1, keepdims=True)
    numbers = jnp.arange(E, dtype=jnp.int32)
    load = jnp.sum((expert_ids[:, :, None] == numbers[None, None, :]).astype(jnp.float32), axis=(0, 1))
    target = jnp.float32(TOKENS * TOPK)
    new_bias = expert_bias + 0.001 * jnp.sign(target - jnp.float32(E) * load)
    return affinities, weights, load, new_bias
```

```python
import functools

import jax
import jax.numpy as jnp
from jax import lax
from jax.experimental import pallas as pl
from jax.experimental.pallas import tpu as pltpu
from jax.sharding import PartitionSpec as P

MESH = pl.DeviceIdType.MESH
F32 = jnp.float32
LINK = jnp.int16
TOP_CODE = 32760.0
TOKEN_BOUND, GATE_BOUND = 6.0, 0.0625
ROOT = 1


def kernel(ntok, widths, x_hbm, w_hbm, ids_hbm, bias_hbm,
           affv, wtsv, load_ref, newb_ref,
           xv, wv, wt, ids, bias_own, bias_all, part, rx1, keep, mine, tx2, rx2, cnt, fin,
           x_sem, w_sem, i_sem, b_sem, s1, r1, s2, r2, sc, rc, sb, rb, sf, rf, ready):
    own = bias_own.shape[1]
    top, rows = ids.shape
    n = len(widths)
    starts = [sum(widths[:i]) for i in range(n)]
    t, e = lax.axis_index("tok"), lax.axis_index("exp")
    y, c = e // 2, e % 2
    mate = 2 * y + 1 - c
    peer = 2 * (1 - y) + c
    experts = 4 * own
    is_root = e == ROOT
    others = [k for k in range(4) if k != ROOT]

    def cols(i):
        return pl.ds(starts[i], widths[i])

    ids_in = pltpu.make_async_copy(ids_hbm, ids, i_sem)
    b_in = pltpu.make_async_copy(bias_hbm, bias_own, b_sem)
    w_in = pltpu.make_async_copy(w_hbm, wv, w_sem)
    x_in = [pltpu.make_async_copy(x_hbm.at[cols(i)], xv.at[cols(i)], x_sem.at[i]) for i in range(n)]
    ids_in.start()
    w_in.start()
    b_in.start()
    ahead = 2
    for copy in x_in[:ahead]:
        copy.start()

    barrier = pltpu.get_barrier_semaphore()

    for k in others:
        @pl.when(e != k)
        def _():
            pl.semaphore_signal(barrier, inc=1, device_id=(t, k), device_id_type=MESH)

    @pl.when(is_root)
    def _():
        for d in range(1, ntok):
            pl.semaphore_signal(barrier, inc=1, device_id=((t + d) % ntok, e), device_id_type=MESH)

    ids_in.wait()
    b_in.wait()

    @pl.when(is_root)
    def _():
        lanes = 128
        numbers = lax.broadcasted_iota(jnp.int32, (experts, lanes), 0).astype(F32).astype(jnp.bfloat16)
        one, zero = jnp.bfloat16(1), jnp.bfloat16(0)
        chunk = 256 // top
        groups = rows // lanes
        total = jnp.zeros((8, experts), F32)
        for g0 in range(0, groups, chunk):
            acc = jnp.zeros((experts, lanes), jnp.bfloat16)
            for g in range(g0, min(g0 + chunk, groups)):
                found = ids[:, pl.ds(g * lanes, lanes)].astype(F32).astype(jnp.bfloat16)
                for j in range(top):
                    acc = acc + jnp.where(found[j:j + 1] == numbers, one, zero)
            total = total + lax.dot_general(jnp.ones((8, lanes), jnp.bfloat16), acc,
                                            (((1,), (1,)), ((), ())), preferred_element_type=F32)
        cnt[0] = total[0:1].astype(jnp.int32)
        bias_all[ROOT] = bias_own[...]

    w_in.wait()
    for copy in x_in[ahead:2 * ahead]:
        copy.start()
    wt[...] = wv[...].T

    bias_out = pltpu.make_async_remote_copy(
        src_ref=bias_own, dst_ref=bias_all.at[e], send_sem=sb, recv_sem=rb.at[e],
        device_id=(t, ROOT), device_id_type=MESH)
    bias_back = [pltpu.make_async_remote_copy(
        src_ref=bias_own, dst_ref=bias_all.at[k], send_sem=sb, recv_sem=rb.at[k],
        device_id=(t, k), device_id_type=MESH) for k in others]
    cnt_out = [pltpu.make_async_remote_copy(
        src_ref=cnt.at[0], dst_ref=cnt.at[d], send_sem=sc.at[d], recv_sem=rc.at[d],
        device_id=((t + d) % ntok, e), device_id_type=MESH) for d in range(1, ntok)]
    fin_out = [pltpu.make_async_remote_copy(
        src_ref=fin, dst_ref=fin, send_sem=sf.at[k], recv_sem=rf,
        device_id=(t, k), device_id_type=MESH) for k in others]

    @pl.when(jnp.logical_not(is_root))
    def _():
        pl.semaphore_wait(barrier, 3)
        pl.semaphore_signal(ready.at[e], inc=1, device_id=(t, ROOT), device_id_type=MESH)
        bias_out.start()

    @pl.when(is_root)
    def _():
        for k in others:
            pl.semaphore_wait(ready.at[k], 1)

    def send_counts():
        pl.semaphore_wait(barrier, ntok - 1)
        for copy in cnt_out:
            copy.start()

    def send_counts_soon():
        pl.when(jnp.logical_and(is_root, 2 * t >= ntok))(send_counts)

    def send_counts_late():
        pl.when(jnp.logical_and(is_root, 2 * t < ntok))(send_counts)

    def finish_counts():
        @pl.when(is_root)
        def _():
            for copy in cnt_out + bias_back:
                copy.wait_recv()
            total = cnt[0]
            for d in range(1, ntok):
                total = total + cnt[d]
            load = total.astype(F32)
            target = F32(ntok * rows * top)
            gap = target - F32(experts) * load
            sign = jnp.where(gap > 0, F32(1), jnp.where(gap < 0, F32(-1), F32(0)))
            bias = jnp.concatenate([bias_all[k] for k in range(4)], axis=1)
            fin[0] = load
            fin[1] = bias + 0.001 * sign
            for copy in fin_out:
                copy.start()

    def close_counts():
        @pl.when(is_root)
        def _():
            for copy in cnt_out + fin_out:
                copy.wait_send()

        @pl.when(jnp.logical_not(is_root))
        def _():
            fin_out[0].wait_recv()
            bias_out.wait_send()

        load_ref[...] = fin[0]
        newb_ref[...] = fin[1]

    def first(i):
        return pltpu.make_async_remote_copy(
            src_ref=part.at[1 - c, :, cols(i)], dst_ref=rx1.at[:, cols(i)],
            send_sem=s1.at[i], recv_sem=r1.at[i], device_id=(t, mate), device_id_type=MESH)

    def second(i):
        return pltpu.make_async_remote_copy(
            src_ref=tx2.at[:, cols(i)], dst_ref=rx2.at[:, cols(i)],
            send_sem=s2.at[i], recv_sem=r2.at[i], device_id=(t, peer), device_id_type=MESH)

    def stage_a(i):
        x_in[i].wait()
        if i + 2 * ahead < n:
            x_in[i + 2 * ahead].start()
        r = lax.dot_general(wt[...], xv[cols(i)], (((1,), (1,)), ((), ())), preferred_element_type=F32)
        for k in range(4):
            part[k % 2, pl.ds(k // 2 * own, own), cols(i)] = r[k * own:(k + 1) * own]
        mine_ids = ids[:, cols(i)]
        low, high = mine_ids & 7, mine_ids >> 3
        picked = jnp.zeros(mine_ids.shape, F32)
        for g in range(experts // 8):
            at = jnp.take_along_axis(r[8 * g:8 * g + 8], low, axis=0, mode="promise_in_bounds")
            picked = jnp.where(high == g, at, picked)
        for k in range(2):
            part[k, pl.ds(2 * own, top), cols(i)] = picked
        first(i).start()

    bound = 2 * xv.shape[1] * TOKEN_BOUND * GATE_BOUND
    grain = TOP_CODE / bound ** 0.25

    def encode(v):
        size = lax.rsqrt(lax.rsqrt(jnp.abs(v) + F32(1e-30))) * F32(grain) + F32(0.5)
        return jnp.where(v < 0, -size, size).astype(jnp.int32)

    def decode(whole):
        u = whole.astype(F32)
        return (u * u * F32(grain ** -4)) * (u * jnp.abs(u))

    def stage_b(i):
        first(i).wait_recv()
        theirs = pl.ds(pl.multiple_of((1 - y) * own, own), own)
        ours = pl.ds(pl.multiple_of(y * own, own), own)
        tops = pl.ds(2 * own, top)
        code = encode(part[c, theirs, cols(i)] + rx1[theirs, cols(i)])
        chosen = encode(part[c, tops, cols(i)] + rx1[tops, cols(i)])
        tx2[0:own, cols(i)] = code.astype(LINK)
        tx2[own:, cols(i)] = chosen.astype(LINK)
        second(i).start()
        keep[:, cols(i)] = part[c, ours, cols(i)] + rx1[ours, cols(i)]
        mine[:, cols(i)] = decode(chosen)

    def stage_c(i):
        second(i).wait_recv()
        code = decode(rx2[0:own, cols(i)].astype(jnp.int32))
        tail = decode(rx2[own:, cols(i)].astype(jnp.int32))
        chosen = 1.0 / (1.0 + jnp.exp(-(mine[:, cols(i)] + tail)))
        wtsv[:, cols(i)] = 2.5 * chosen / jnp.sum(chosen, axis=0, keepdims=True)
        affv[:, cols(i)] = 1.0 / (1.0 + jnp.exp(-(keep[:, cols(i)] + code)))

    lag_b = 3
    for step in range(n + lag_b):
        if step < n:
            stage_a(step)
        if step == lag_b - 1:
            send_counts_soon()
        if 0 <= step - lag_b < n:
            stage_b(step - lag_b)
    send_counts_late()
    for i in range(n):
        if i == n - 2:
            finish_counts()
        stage_c(i)
    close_counts()
    for i in range(n):
        first(i).wait_send()
        second(i).wait_send()


def place(aff, wts, load, newb, aff_hbm, wts_hbm, load_hbm, newb_hbm, sem):
    copies = [pltpu.make_async_copy(a, b, sem.at[k]) for k, (a, b) in enumerate(
        ((aff, aff_hbm), (wts, wts_hbm), (load, load_hbm), (newb, newb_hbm)))]
    for copy in copies:
        copy.start()
    for copy in copies:
        copy.wait()


def local(ntok, tokens, gate_weight, expert_ids, expert_bias):
    rows, depth = tokens.shape
    experts = gate_weight.shape[1]
    own = expert_bias.shape[0]
    top = expert_ids.shape[1]
    piece = 256
    widths = [piece // 2] * 2 + [piece] * (rows // piece - 1)
    n = len(widths)
    dma = pltpu.SemaphoreType.DMA
    vm = pltpu.VMEM
    any_ = pl.BlockSpec(memory_space=pl.ANY)
    vmem = pl.BlockSpec(memory_space=pltpu.VMEM)
    shapes = ((own, rows), (top, rows), (1, experts), (1, experts))
    results = pl.pallas_call(
        functools.partial(kernel, ntok, widths),
        out_shape=tuple(pltpu.VMEM(shape, F32) for shape in shapes),
        in_specs=[any_] * 4,
        out_specs=(vmem,) * 4,
        scratch_shapes=[
            vm((rows, depth), tokens.dtype), vm((depth, experts), gate_weight.dtype),
            vm((experts, depth), gate_weight.dtype), vm((top, rows), jnp.int32),
            vm((1, own), F32), vm((4, 1, own), F32),
            vm((2, 2 * own + top, rows), F32), vm((2 * own + top, rows), F32),
            vm((own, rows), F32), vm((top, rows), F32),
            vm((own + top, rows), LINK), vm((own + top, rows), LINK),
            vm((ntok, 1, experts), jnp.int32), vm((2, 1, experts), F32),
            dma((n,)), dma, dma, dma, dma((n,)), dma((n,)), dma((n,)), dma((n,)),
            dma((ntok,)), dma((ntok,)), dma, dma((4,)), dma((4,)), dma,
            pltpu.SemaphoreType.REGULAR((4,)),
        ],
        compiler_params=pltpu.CompilerParams(
            collective_id=0, has_side_effects=True, vmem_limit_bytes=60 * 1024 * 1024),
    )(tokens, gate_weight, expert_ids.T, expert_bias.reshape(1, own))
    aff, wts, load, newb = pl.pallas_call(
        place,
        out_shape=tuple(jax.ShapeDtypeStruct(shape, F32) for shape in shapes),
        in_specs=[vmem] * 4,
        out_specs=(pl.BlockSpec(memory_space=pltpu.HBM),) * 4,
        scratch_shapes=[dma((4,))],
    )(*(pltpu.with_memory_space_constraint(r, pltpu.VMEM) for r in results))
    return aff.T, wts.T, load.reshape(experts), newb.reshape(experts)


def solution(mesh):
    in_specs = (P("tok", "exp"), P("exp", None), P("tok", None), P("exp"))
    out_specs = (P("tok", "exp"), P("tok", None), P(), P())
    return jax.shard_map(functools.partial(local, mesh.shape["tok"]), mesh=mesh,
                         in_specs=in_specs, out_specs=out_specs, check_vma=False)
```

```python
import functools

import jax
import jax.numpy as jnp
from jax import lax
from jax.experimental import pallas as pl
from jax.experimental.pallas import tpu as pltpu
from jax.sharding import PartitionSpec as P

MESH = pl.DeviceIdType.MESH
F32 = jnp.float32
LINK = jnp.int16
TOP_CODE = 32760.0
TOKEN_BOUND, GATE_BOUND = 6.0, 0.0625
W_CHUNKS = 4
ROOT = 1


def plan(n, ahead):
    order = [("a", i) for i in range(ahead)]
    for i in range(n):
        order += [("b", i)] + ([("a", i + ahead)] if i + ahead < n else [])
    return order


def kernel(ntok, widths, x_hbm, w_hbm, ids_hbm, bias_hbm,
           affv, wtsv, load_ref, newb_ref,
           xv, wv, ids, bias_all, part, rx1, keep, mine, tx2, rx2, cnt, fin,
           l_sem, s1, r1, s2, r2, sc, rc, rb, ready):
    sizes = sorted(set(widths))
    acc_of = []
    for i, width in enumerate(widths):
        acc_of.append(2 * sizes.index(width) + sum(w == width for w in widths[:i]) % 2)
    specs = [tuple(pltpu.ACC(q)((width, 256), F32) for q in (0, 1)) for width in sizes for _ in range(2)]
    pl.run_scoped(functools.partial(body, ntok, widths, acc_of, (
        x_hbm, w_hbm, ids_hbm, bias_hbm, affv, wtsv, load_ref, newb_ref,
        xv, wv, ids, bias_all, part, rx1, keep, mine, tx2, rx2, cnt, fin,
        l_sem, s1, r1, s2, r2, sc, rc, rb, ready)), *specs)


def body(ntok, widths, acc_of, refs, *accs):
    (x_hbm, w_hbm, ids_hbm, bias_hbm, affv, wtsv, load_ref, newb_ref,
     xv, wv, ids, bias_all, part, rx1, keep, mine, tx2, rx2, cnt, fin,
     l_sem, s1, r1, s2, r2, sc, rc, rb, ready) = refs
    own = bias_all.shape[2]
    top, rows = ids.shape
    depth = xv.shape[1]
    n = len(widths)
    starts = [sum(widths[:i]) for i in range(n)]
    t, e = lax.axis_index("tok"), lax.axis_index("exp")
    y, c = e // 2, e % 2
    mate = 2 * y + 1 - c
    peer = 2 * (1 - y) + c
    experts = 4 * own
    is_root = e == ROOT
    others = [k for k in range(4) if k != ROOT]

    def cols(i):
        return pl.ds(starts[i], widths[i])

    chunk = -(-depth // W_CHUNKS // 256) * 256
    chunks = [pl.ds(k, min(chunk, depth - k)) for k in range(0, depth, chunk)]
    nw = len(chunks)
    w_in = [pltpu.make_async_copy(w_hbm.at[k], wv.at[k], l_sem.at[j]) for j, k in enumerate(chunks)]
    first_x = 3
    slot = [nw + i if i < first_x else (i - first_x) % (nw + first_x) for i in range(n)]
    x_in = [pltpu.make_async_copy(x_hbm.at[cols(i)], xv.at[cols(i)], l_sem.at[slot[i]]) for i in range(n)]
    ids_in = pltpu.make_async_copy(ids_hbm, ids, l_sem.at[nw + first_x])
    ids_in.start()
    for copy in w_in + x_in[:first_x]:
        copy.start()

    barrier = pltpu.get_barrier_semaphore()

    for k in others:
        @pl.when(e != k)
        def _():
            pl.semaphore_signal(barrier, inc=1, device_id=(t, k), device_id_type=MESH)

    bias_in = pltpu.make_async_copy(bias_hbm, bias_all.at[ROOT], sc)
    bias_out = pltpu.make_async_remote_copy(
        src_ref=bias_hbm, dst_ref=bias_all.at[e], send_sem=sc, recv_sem=rb,
        device_id=(t, ROOT), device_id_type=MESH)
    bias_back = pltpu.make_async_remote_copy(
        src_ref=bias_all.at[pl.ds(0, 3)], dst_ref=bias_all.at[pl.ds(0, 3)], send_sem=sc, recv_sem=rb,
        device_id=(t, mate), device_id_type=MESH)
    cnt_out = [pltpu.make_async_remote_copy(
        src_ref=cnt.at[0], dst_ref=cnt.at[d], send_sem=sc, recv_sem=rc,
        device_id=((t + d) % ntok, e), device_id_type=MESH) for d in range(1, ntok)]
    rest = pl.ds(1, ntok - 1)
    cnt_all = pltpu.make_async_remote_copy(
        src_ref=cnt.at[rest], dst_ref=cnt.at[rest], send_sem=sc, recv_sem=rc,
        device_id=(t, mate), device_id_type=MESH)
    fin_out = [pltpu.make_async_remote_copy(
        src_ref=fin.at[j], dst_ref=fin.at[3], send_sem=sc, recv_sem=rc,
        device_id=(t, k), device_id_type=MESH) for j, k in enumerate(others)]
    fin_all = pltpu.make_async_remote_copy(
        src_ref=fin.at[pl.ds(0, 3)], dst_ref=fin.at[pl.ds(0, 3)], send_sem=sc, recv_sem=rc,
        device_id=(t, mate), device_id_type=MESH)

    @pl.when(is_root)
    def _():
        bias_in.start()
        for d in range(1, ntok):
            pl.semaphore_signal(barrier, inc=1, device_id=((t + d) % ntok, e), device_id_type=MESH)
        ids_in.wait()
        lanes = 128
        numbers = lax.broadcasted_iota(jnp.int32, (experts, lanes), 0).astype(F32).astype(jnp.bfloat16)
        one, zero = jnp.bfloat16(1), jnp.bfloat16(0)
        exact = 256 // top
        blocks = rows // lanes
        total = jnp.zeros((1, experts), F32)
        for g0 in range(0, blocks, exact):
            acc = jnp.zeros((experts, lanes), jnp.bfloat16)
            for g in range(g0, min(g0 + exact, blocks)):
                found = ids[:, pl.ds(g * lanes, lanes)].astype(F32).astype(jnp.bfloat16)
                for j in range(top):
                    acc = acc + jnp.where(found[j:j + 1] == numbers, one, zero)
            total = total + jnp.sum(acc.astype(F32).T, axis=0, keepdims=True)
        cnt[0] = total.astype(jnp.int32)
        bias_in.wait()

    @pl.when(jnp.logical_not(is_root))
    def _():
        pl.semaphore_wait(barrier, 3)
        pl.semaphore_signal(ready, inc=1, device_id=(t, ROOT), device_id_type=MESH)
        bias_out.start()
        ids_in.wait()

    queue = list(range(first_x, n))

    def more_tokens(freed):
        while queue and slot[queue[0]] in freed:
            x_in[queue.pop(0)].start()

    def send_counts():
        pl.semaphore_wait(barrier, ntok - 1)
        for copy in cnt_out:
            copy.start()

    def send_counts_soon():
        pl.when(jnp.logical_and(is_root, 2 * t >= ntok))(send_counts)

    def send_counts_late():
        pl.when(jnp.logical_and(is_root, 2 * t < ntok))(send_counts)

    def finish_counts():
        @pl.when(is_root)
        def _():
            cnt_all.wait()
            bias_back.wait_recv()
            total = cnt[0]
            for d in range(1, ntok):
                total = total + cnt[d]
            load = total.astype(F32)
            target = F32(ntok * rows * top)
            gap = target - F32(experts) * load
            sign = jnp.where(gap > 0, F32(1), jnp.where(gap < 0, F32(-1), F32(0)))
            bias = jnp.concatenate([bias_all[k] for k in range(4)], axis=1)
            for j in range(4):
                fin[j, 0] = load
                fin[j, 1] = bias + 0.001 * sign
            for copy in fin_out:
                copy.start()

    def close_counts():
        @pl.when(is_root)
        def _():
            fin_all.wait_send()

        @pl.when(jnp.logical_not(is_root))
        def _():
            fin_out[0].wait_recv()
            bias_out.wait_send()

        load_ref[...] = fin[3, 0]
        newb_ref[...] = fin[3, 1]

    def first(at, i):
        return pltpu.make_async_remote_copy(
            src_ref=part.at[1 - c, :, at], dst_ref=rx1.at[:, at],
            send_sem=s1, recv_sem=r1.at[i], device_id=(t, mate), device_id_type=MESH)

    def second(at, i):
        return pltpu.make_async_remote_copy(
            src_ref=tx2.at[:, at], dst_ref=rx2.at[:, at],
            send_sem=s2, recv_sem=r2.at[i], device_id=(t, peer), device_id_type=MESH)

    side = 256
    tiles = depth // side
    shares = [[(q, k) for q in (0, 1) for k in range(tiles)
               if (k < (tiles + 1 - i % 2) // 2) == (q == 0)] for i in range(n)]
    line = [[(i, k) for i in range(n) for p, k in shares[i] if p == q] for q in (0, 1)]
    where = [0, 0]

    def push(q):
        if where[q] < len(line[q]):
            k = line[q][where[q]][1]
            pltpu.matmul_push_rhs(wv[pl.ds(k * side, side), :], staging_register=where[q] % 2, mxu_index=q)

    def issue(i):
        x_in[i].wait()
        more_tokens([slot[i]])
        left = [[k for p, k in shares[i] if p == q] for q in (0, 1)]
        for step in range(max(map(len, left))):
            for q in (0, 1):
                if step < len(left[q]):
                    k = left[q][step]
                    mark = where[q] % 2
                    where[q] += 1
                    push(q)
                    pltpu.matmul_acc_lhs(accs[acc_of[i]][q], xv[cols(i), pl.ds(k * side, side)], load_staged_rhs=mark)

    def stage_a(i):
        if i + 1 < n:
            issue(i + 1)
        r = (pltpu.matmul_pop(accs[acc_of[i]][0]) + pltpu.matmul_pop(accs[acc_of[i]][1])).T
        for k in range(4):
            part[k % 2, pl.ds(k // 2 * own, own), cols(i)] = r[k * own:(k + 1) * own]
        mine_ids = ids[:, cols(i)]
        low, high = mine_ids & 7, mine_ids >> 3
        picked = jnp.zeros(mine_ids.shape, F32)
        for k in range(experts // 8):
            row = jnp.take_along_axis(r[8 * k:8 * k + 8], low, axis=0, mode="promise_in_bounds")
            picked = jnp.where(high == k, row, picked)
        for k in range(2):
            part[k, pl.ds(2 * own, top), cols(i)] = picked
        if i == 0:
            @pl.when(is_root)
            def _():
                pl.semaphore_wait(ready, 3)
        first(cols(i), i).start()

    bound = 2 * depth * TOKEN_BOUND * GATE_BOUND
    grain = TOP_CODE / bound ** 0.25

    def encode(v):
        size = lax.rsqrt(lax.rsqrt(jnp.abs(v) + F32(1e-30))) * F32(grain) + F32(0.5)
        return jnp.where(v < 0, -size, size).astype(jnp.int32)

    def decode(whole):
        u = whole.astype(F32)
        return (u * u * F32(grain ** -4)) * (u * jnp.abs(u))

    def stage_b(i):
        first(cols(i), i).wait_recv()
        theirs = pl.ds(pl.multiple_of((1 - y) * own, own), own)
        ours = pl.ds(pl.multiple_of(y * own, own), own)
        tops = pl.ds(2 * own, top)
        code = encode(part[c, theirs, cols(i)] + rx1[theirs, cols(i)])
        chosen = encode(part[c, tops, cols(i)] + rx1[tops, cols(i)])
        tx2[0:own, cols(i)] = code.astype(LINK)
        tx2[own:, cols(i)] = chosen.astype(LINK)
        second(cols(i), i).start()
        keep[:, cols(i)] = part[c, ours, cols(i)] + rx1[ours, cols(i)]
        mine[:, cols(i)] = decode(chosen)

    def stage_c(i):
        second(cols(i), i).wait_recv()
        code = decode(rx2[0:own, cols(i)].astype(jnp.int32))
        tail = decode(rx2[own:, cols(i)].astype(jnp.int32))
        chosen = 1.0 / (1.0 + jnp.exp(-(mine[:, cols(i)] + tail)))
        wtsv[:, cols(i)] = 2.5 * chosen / jnp.sum(chosen, axis=0, keepdims=True)
        affv[:, cols(i)] = 1.0 / (1.0 + jnp.exp(-(keep[:, cols(i)] + code)))

    for j, copy in enumerate(w_in):
        copy.wait()
        more_tokens([j])
    for q in (0, 1):
        push(q)
    issue(0)
    for kind, i in plan(n, 3):
        if kind == "a":
            stage_a(i)
        else:
            stage_b(i)
        if (kind, i) == ("a", 1):
            send_counts_soon()
        if (kind, i) == ("a", n - 1):
            send_counts_late()
    for i in range(n):
        if i == n - 2:
            finish_counts()
        stage_c(i)
    close_counts()
    every = pl.ds(0, rows)
    first(every, 0).wait_send()
    second(every, 0).wait_send()


def place(aff, wts, load, newb, aff_hbm, wts_hbm, load_hbm, newb_hbm, sem):
    copies = [pltpu.make_async_copy(a, b, sem.at[k]) for k, (a, b) in enumerate(
        ((aff, aff_hbm), (wts, wts_hbm), (load, load_hbm), (newb, newb_hbm)))]
    for copy in copies:
        copy.start()
    for copy in copies:
        copy.wait()


def local(ntok, tokens, gate_weight, expert_ids, expert_bias):
    rows, depth = tokens.shape
    experts = gate_weight.shape[1]
    own = expert_bias.shape[0]
    top = expert_ids.shape[1]
    piece = 256
    widths = [piece // 2] * 2 + [piece] * (rows // piece - 1)
    n = len(widths)
    dma = pltpu.SemaphoreType.DMA
    vm = pltpu.VMEM
    any_ = pl.BlockSpec(memory_space=pl.ANY)
    vmem = pl.BlockSpec(memory_space=pltpu.VMEM)
    shapes = ((own, rows), (top, rows), (1, experts), (1, experts))
    results = pl.pallas_call(
        functools.partial(kernel, ntok, widths),
        out_shape=tuple(pltpu.VMEM(shape, F32) for shape in shapes),
        in_specs=[any_] * 4,
        out_specs=(vmem,) * 4,
        scratch_shapes=[
            vm((rows, depth), tokens.dtype), vm((depth, experts), gate_weight.dtype),
            vm((top, rows), jnp.int32),
            vm((4, 1, own), F32),
            vm((2, 2 * own + top, rows), F32), vm((2 * own + top, rows), F32),
            vm((own, rows), F32), vm((top, rows), F32),
            vm((own + top, rows), LINK), vm((own + top, rows), LINK),
            vm((ntok, 1, experts), jnp.int32), vm((4, 2, 1, experts), F32),
            dma((W_CHUNKS + 4,)), dma, dma((n,)), dma, dma((n,)), dma, dma, dma, pltpu.SemaphoreType.REGULAR,
        ],
        compiler_params=pltpu.CompilerParams(
            collective_id=0, has_side_effects=True, vmem_limit_bytes=60 * 1024 * 1024),
    )(tokens, gate_weight, expert_ids.T, expert_bias.reshape(1, own))
    aff, wts, load, newb = pl.pallas_call(
        place,
        out_shape=tuple(jax.ShapeDtypeStruct(shape, F32) for shape in shapes),
        in_specs=[vmem] * 4,
        out_specs=(pl.BlockSpec(memory_space=pltpu.HBM),) * 4,
        scratch_shapes=[dma((4,))],
    )(*(pltpu.with_memory_space_constraint(r, pltpu.VMEM) for r in results))
    return aff.T, wts.T, load.reshape(experts), newb.reshape(experts)


def solution(mesh):
    in_specs = (P("tok", "exp"), P("exp", None), P("tok", None), P("exp"))
    out_specs = (P("tok", "exp"), P("tok", None), P(), P())
    return jax.shard_map(functools.partial(local, mesh.shape["tok"]), mesh=mesh,
                         in_specs=in_specs, out_specs=out_specs, check_vma=False)
```

```python
import functools

import jax
import jax.numpy as jnp
from jax import lax
from jax.experimental import pallas as pl
from jax.experimental.pallas import tpu as pltpu
from jax.sharding import PartitionSpec as P

MESH = pl.DeviceIdType.MESH
F32 = jnp.float32
LINK = jnp.int16
TOP_CODE = 32760.0
TOKEN_BOUND, GATE_BOUND = 6.0, 0.0625
W_CHUNKS = 4
LAG = (2, 5)
HELD = 4
AHEAD = 4
ROOT = 1


def plan(n):
    turn = list(range(1, n))
    turn.insert(min(3, n - 1), 0)
    order = []
    for i in range(n + max(LAG)):
        if i < n:
            order.append(("a", i))
        order += [(core, turn[i - LAG[core]]) for core in (0, 1) if 0 <= i - LAG[core] < n]
    return order


def kernel(ntok, widths, x_hbm, w_hbm, ids_hbm, bias_hbm,
           affv, wtsv, load_ref, newb_ref,
           xv, wv, ids, bias_all, part, rx1, keep, mine, tx2, rx2, tx3, rx3, cnt, fin,
           l_sem, s1, r1, s2, r2, s3, r3, sc, rc, rb, ready):
    units = [widths[0] // 2] * 2 + widths[1:]
    sizes = sorted(set(units))
    acc_of = [2 * sizes.index(unit) + sum(u == unit for u in units[:j]) % 2 for j, unit in enumerate(units)]
    specs = [tuple(pltpu.ACC(q)((width, 256), F32) for q in (0, 1)) for width in sizes for _ in range(2)]
    pl.run_scoped(functools.partial(body, ntok, widths, units, acc_of, (
        x_hbm, w_hbm, ids_hbm, bias_hbm, affv, wtsv, load_ref, newb_ref,
        xv, wv, ids, bias_all, part, rx1, keep, mine, tx2, rx2, tx3, rx3, cnt, fin,
        l_sem, s1, r1, s2, r2, s3, r3, sc, rc, rb, ready)), *specs)


def body(ntok, widths, units, acc_of, refs, *accs):
    (x_hbm, w_hbm, ids_hbm, bias_hbm, affv, wtsv, load_ref, newb_ref,
     xv, wv, ids, bias_all, part, rx1, keep, mine, tx2, rx2, tx3, rx3, cnt, fin,
     l_sem, s1, r1, s2, r2, s3, r3, sc, rc, rb, ready) = refs
    own = bias_all.shape[2]
    top, rows = ids.shape
    depth = xv.shape[1]
    n = len(widths)
    starts = [sum(widths[:i]) for i in range(n)]
    t, e = lax.axis_index("tok"), lax.axis_index("exp")
    y, c = e // 2, e % 2
    mate = 2 * y + 1 - c
    peer = 2 * (1 - y) + c
    cross = 2 * (1 - y) + 1 - c
    experts = 4 * own
    is_root = e == ROOT
    others = [k for k in range(4) if k != ROOT]

    def cols(i):
        return pl.ds(starts[i], widths[i])

    nu = len(units)

    def unit(j):
        return pl.ds(sum(units[:j]), units[j])

    chunk = -(-depth // W_CHUNKS // 256) * 256
    chunks = [pl.ds(k, min(chunk, depth - k)) for k in range(0, depth, chunk)]
    w_in = [pltpu.make_async_copy(w_hbm.at[k], wv.at[k], l_sem.at[0]) for k in chunks]
    w_all = pltpu.make_async_copy(w_hbm, wv, l_sem.at[0])
    ids_in = pltpu.make_async_copy(ids_hbm, ids, l_sem.at[1])
    slot = [2 + i if i < AHEAD else 0 if i == AHEAD else 2 + (i - AHEAD - 1) % AHEAD for i in range(nu)]
    x_in = [pltpu.make_async_copy(x_hbm.at[unit(j)], xv.at[unit(j)], l_sem.at[slot[j]]) for j in range(nu)]
    ids_in.start()
    for copy in w_in + x_in[:AHEAD]:
        copy.start()

    barrier = pltpu.get_barrier_semaphore()

    for k in others:
        @pl.when(e != k)
        def _():
            pl.semaphore_signal(barrier, inc=1, device_id=(t, k), device_id_type=MESH)

    bias_in = pltpu.make_async_copy(bias_hbm, bias_all.at[ROOT], sc)
    bias_out = pltpu.make_async_remote_copy(
        src_ref=bias_hbm, dst_ref=bias_all.at[e], send_sem=sc, recv_sem=rb,
        device_id=(t, ROOT), device_id_type=MESH)
    bias_back = pltpu.make_async_remote_copy(
        src_ref=bias_all.at[pl.ds(0, 3)], dst_ref=bias_all.at[pl.ds(0, 3)], send_sem=sc, recv_sem=rb,
        device_id=(t, mate), device_id_type=MESH)
    cnt_out = [pltpu.make_async_remote_copy(
        src_ref=cnt.at[0], dst_ref=cnt.at[d], send_sem=sc, recv_sem=rc,
        device_id=((t + d) % ntok, e), device_id_type=MESH) for d in range(1, ntok)]
    rest = pl.ds(1, ntok - 1)
    cnt_all = pltpu.make_async_remote_copy(
        src_ref=cnt.at[rest], dst_ref=cnt.at[rest], send_sem=sc, recv_sem=rc,
        device_id=(t, mate), device_id_type=MESH)
    fin_out = [pltpu.make_async_remote_copy(
        src_ref=fin.at[j], dst_ref=fin.at[3], send_sem=sc, recv_sem=rc,
        device_id=(t, k), device_id_type=MESH) for j, k in enumerate(others)]
    fin_all = pltpu.make_async_remote_copy(
        src_ref=fin.at[pl.ds(0, 3)], dst_ref=fin.at[pl.ds(0, 3)], send_sem=sc, recv_sem=rc,
        device_id=(t, mate), device_id_type=MESH)

    @pl.when(is_root)
    def _():
        bias_in.start()
        for d in range(1, ntok):
            pl.semaphore_signal(barrier, inc=1, device_id=((t + d) % ntok, e), device_id_type=MESH)
        ids_in.wait()
        lanes = 128
        numbers = lax.broadcasted_iota(jnp.int32, (experts, lanes), 0).astype(F32).astype(jnp.bfloat16)
        one, zero = jnp.bfloat16(1), jnp.bfloat16(0)
        exact = 256 // top
        blocks = rows // lanes
        total = jnp.zeros((1, experts), F32)
        for g0 in range(0, blocks, exact):
            acc = jnp.zeros((experts, lanes), jnp.bfloat16)
            for g in range(g0, min(g0 + exact, blocks)):
                found = ids[:, pl.ds(g * lanes, lanes)].astype(F32).astype(jnp.bfloat16)
                for j in range(top):
                    acc = acc + jnp.where(found[j:j + 1] == numbers, one, zero)
            total = total + jnp.sum(acc.astype(F32).T, axis=0, keepdims=True)
        cnt[0] = total.astype(jnp.int32)
        bias_in.wait()

    @pl.when(jnp.logical_not(is_root))
    def _():
        pl.semaphore_wait(barrier, 3)
        pl.semaphore_signal(ready, inc=1, device_id=(t, ROOT), device_id_type=MESH)
        bias_out.start()
        ids_in.wait()

    queue = list(range(AHEAD, nu))

    def more_tokens(freed):
        if queue and slot[queue[0]] == freed:
            x_in[queue.pop(0)].start()

    def send_counts():
        pl.semaphore_wait(barrier, ntok - 1)
        for copy in cnt_out:
            copy.start()

    def send_counts_soon():
        pl.when(jnp.logical_and(is_root, 2 * t >= ntok))(send_counts)

    def send_counts_late():
        pl.when(jnp.logical_and(is_root, 2 * t < ntok))(send_counts)

    def finish_counts():
        @pl.when(is_root)
        def _():
            cnt_all.wait()
            bias_back.wait_recv()
            total = cnt[0]
            for d in range(1, ntok):
                total = total + cnt[d]
            load = total.astype(F32)
            target = F32(ntok * rows * top)
            gap = target - F32(experts) * load
            sign = jnp.where(gap > 0, F32(1), jnp.where(gap < 0, F32(-1), F32(0)))
            bias = jnp.concatenate([bias_all[k] for k in range(4)], axis=1)
            for j in range(4):
                fin[j, 0] = load
                fin[j, 1] = bias + 0.001 * sign
            for copy in fin_out:
                copy.start()

    def close_counts():
        @pl.when(is_root)
        def _():
            fin_all.wait_send()

        @pl.when(jnp.logical_not(is_root))
        def _():
            fin_out[0].wait_recv()
            bias_out.wait_send()

        load_ref[...] = fin[3, 0]
        newb_ref[...] = fin[3, 1]

    def first(at, i):
        return pltpu.make_async_remote_copy(
            src_ref=part.at[1 - c, :, at], dst_ref=rx1.at[:, at],
            send_sem=s1, recv_sem=r1.at[i], device_id=(t, mate), device_id_type=MESH)

    def second(at, i):
        return pltpu.make_async_remote_copy(
            src_ref=tx2.at[:, at], dst_ref=rx2.at[:, at],
            send_sem=s2, recv_sem=r2.at[i], device_id=(t, peer), device_id_type=MESH)

    def across(j):
        at = pl.ds(rows + sum(units[:j]), units[j])
        return pltpu.make_async_remote_copy(
            src_ref=tx2.at[:, at], dst_ref=rx2.at[:, at],
            send_sem=s2, recv_sem=r2.at[0], device_id=(t, cross), device_id_type=MESH)

    chosen_out = pltpu.make_async_remote_copy(
        src_ref=tx3, dst_ref=rx3, send_sem=s3, recv_sem=r3, device_id=(t, peer), device_id_type=MESH)
    hand_on = pltpu.make_async_remote_copy(
        src_ref=rx3, dst_ref=rx3, send_sem=s3, recv_sem=r3, device_id=(t, mate), device_id_type=MESH)

    side = 256
    tiles = depth // side
    shares = [[(q, k) for q in (0, 1) for k in range(tiles)
               if (k < (tiles + 1 - i % 2) // 2) == (q == 0)] for i in range(nu)]
    line = [[(i, k) for i in range(nu) for p, k in shares[i] if p == q] for q in (0, 1)]
    where = [0, 0]

    def push(q):
        if where[q] < len(line[q]):
            k = line[q][where[q]][1]
            pltpu.matmul_push_rhs(wv[pl.ds(k * side, side), :], staging_register=where[q] % 2, mxu_index=q)

    def issue(i):
        x_in[i].wait()
        more_tokens(slot[i])
        left = [[k for p, k in shares[i] if p == q] for q in (0, 1)]
        for step in range(max(map(len, left))):
            for q in (0, 1):
                if step < len(left[q]):
                    k = left[q][step]
                    mark = where[q] % 2
                    where[q] += 1
                    push(q)
                    pltpu.matmul_acc_lhs(accs[acc_of[i]][q], xv[unit(i), pl.ds(k * side, side)], load_staged_rhs=mark)

    def product(j):
        at = unit(j)
        if j + 1 < nu:
            issue(j + 1)
        r = (pltpu.matmul_pop(accs[acc_of[j]][0]) + pltpu.matmul_pop(accs[acc_of[j]][1])).T
        for k in range(4):
            part[k % 2, pl.ds(k // 2 * own, own), at] = r[k * own:(k + 1) * own]

    def pick(at):
        mine_ids = ids[:, at]
        low, high = mine_ids & 7, mine_ids >> 3
        picked = jnp.zeros(mine_ids.shape, F32)
        for k in range(experts // 8):
            block, line = divmod(8 * k, own)
            rows8 = part[block % 2, pl.ds(block // 2 * own + line, 8), at]
            row = jnp.take_along_axis(rows8, low, axis=0, mode="promise_in_bounds")
            picked = jnp.where(high == k, row, picked)
        for k in range(2):
            part[k, pl.ds(2 * own, top), at] = picked

    def to_mate(i):
        pick(cols(i))
        first(cols(i), i).start()

    def stage_a(i):
        if i == 0:
            for j in (0, 1):
                product(j)
                if j == 0:
                    @pl.when(is_root)
                    def _():
                        pl.semaphore_wait(ready, 3)
                tx2[:, unit(j)] = encode(part[c, theirs, unit(j)]).astype(LINK)
                tx2[:, pl.ds(rows + sum(units[:j]), units[j])] = encode(part[1 - c, theirs, unit(j)]).astype(LINK)
                second(unit(j), 0).start()
                across(j).start()
        else:
            product(i + 1)
            to_mate(i)
        if i == 1:
            to_mate(0)

    bound = 2 * depth * TOKEN_BOUND * GATE_BOUND
    grain = TOP_CODE / bound ** 0.25

    def encode(v):
        size = lax.rsqrt(lax.rsqrt(jnp.abs(v) + F32(1e-30))) * F32(grain) + F32(0.5)
        return jnp.where(v < 0, -size, size).astype(jnp.int32)

    def decode(whole):
        u = whole.astype(F32)
        return (u * u * F32(grain ** -4)) * (u * jnp.abs(u))

    theirs = pl.ds(pl.multiple_of((1 - y) * own, own), own)
    ours = pl.ds(pl.multiple_of(y * own, own), own)
    picks = pl.ds(2 * own, top)

    def stage_b(i, core):
        first(cols(i), i).wait_recv()
        if i > 0:
            tx2[:, cols(i)] = encode(part[c, theirs, cols(i)] + rx1[theirs, cols(i)]).astype(LINK)
            if core == 0 or i < n - HELD:
                second(cols(i), i).start()
        chosen = encode(part[c, picks, cols(i)] + rx1[picks, cols(i)])
        if core == 1:
            tx3[:, cols(i)] = chosen.astype(LINK)
        if core == 1 and i == n - 1:
            chosen_out.start()
            for k in range(n - HELD, n):
                second(cols(k), k).start()
        keep[:, cols(i)] = part[c, ours, cols(i)] + rx1[ours, cols(i)]
        mine[:, cols(i)] = decode(chosen)

    def weigh():
        chosen = 1.0 / (1.0 + jnp.exp(-(mine[...] + decode(rx3[...].astype(jnp.int32)))))
        wtsv[...] = 2.5 * chosen / jnp.sum(chosen, axis=0, keepdims=True)

    def stage_c(i):
        second(pl.ds(0, 2 * widths[0]) if i == 0 else cols(i), i).wait_recv()
        logits = keep[:, cols(i)] + decode(rx2[:, cols(i)].astype(jnp.int32))
        if i == 0:
            logits = logits + decode(rx2[:, pl.ds(rows, widths[0])].astype(jnp.int32))
        affv[:, cols(i)] = 1.0 / (1.0 + jnp.exp(-logits))

    w_all.wait()
    more_tokens(0)
    for q in (0, 1):
        push(q)
    issue(0)
    for kind, i in plan(n):
        if kind == "a":
            stage_a(i)
        else:
            pl.when(c == kind)(functools.partial(stage_b, i, kind))
        if (kind, i) == ("a", 1):
            send_counts_soon()
        if (kind, i) == ("a", n - 1):
            send_counts_late()
    for i in range(n):
        if i == n - HELD:
            @pl.when(c == 1)
            def _():
                chosen_out.wait()
                hand_on.start()
            finish_counts()
        if i == n - 1:
            pl.when(c == 0)(hand_on.wait_recv)
            weigh()
        stage_c(i)
    close_counts()
    first(pl.ds(0, rows), 0).wait_send()
    second(pl.ds(0, rows + widths[0]), 0).wait_send()
    pl.when(c == 1)(hand_on.wait_send)


def place(aff, wts, load, newb, aff_hbm, wts_hbm, load_hbm, newb_hbm, sem):
    copies = [pltpu.make_async_copy(a, b, sem.at[k]) for k, (a, b) in enumerate(
        ((aff, aff_hbm), (wts, wts_hbm), (load, load_hbm), (newb, newb_hbm)))]
    for copy in copies:
        copy.start()
    for copy in copies:
        copy.wait()


def local(ntok, tokens, gate_weight, expert_ids, expert_bias):
    rows, depth = tokens.shape
    experts = gate_weight.shape[1]
    own = expert_bias.shape[0]
    top = expert_ids.shape[1]
    piece = 256
    widths = [piece] * (rows // piece)
    n = len(widths)
    dma = pltpu.SemaphoreType.DMA
    vm = pltpu.VMEM
    any_ = pl.BlockSpec(memory_space=pl.ANY)
    vmem = pl.BlockSpec(memory_space=pltpu.VMEM)
    shapes = ((own, rows), (top, rows), (1, experts), (1, experts))
    results = pl.pallas_call(
        functools.partial(kernel, ntok, widths),
        out_shape=tuple(pltpu.VMEM(shape, F32) for shape in shapes),
        in_specs=[any_] * 4,
        out_specs=(vmem,) * 4,
        scratch_shapes=[
            vm((rows, depth), tokens.dtype), vm((depth, experts), gate_weight.dtype),
            vm((top, rows), jnp.int32),
            vm((4, 1, own), F32),
            vm((2, 2 * own + top, rows), F32), vm((2 * own + top, rows), F32),
            vm((own, rows), F32), vm((top, rows), F32),
            vm((own, rows + piece), LINK), vm((own, rows + piece), LINK),
            vm((top, rows), LINK), vm((top, rows), LINK),
            vm((ntok, 1, experts), jnp.int32), vm((4, 2, 1, experts), F32),
            dma((2 + AHEAD,)), dma, dma((n,)), dma, dma((n,)), dma, dma, dma, dma, dma,
            pltpu.SemaphoreType.REGULAR,
        ],
        compiler_params=pltpu.CompilerParams(
            collective_id=0, has_side_effects=True, vmem_limit_bytes=60 * 1024 * 1024),
    )(tokens, gate_weight, expert_ids.T, expert_bias.reshape(1, own))
    aff, wts, load, newb = pl.pallas_call(
        place,
        out_shape=tuple(jax.ShapeDtypeStruct(shape, F32) for shape in shapes),
        in_specs=[vmem] * 4,
        out_specs=(pl.BlockSpec(memory_space=pltpu.HBM),) * 4,
        scratch_shapes=[dma((4,))],
    )(*(pltpu.with_memory_space_constraint(r, pltpu.VMEM) for r in results))
    return aff.T, wts.T, load.reshape(experts), newb.reshape(experts)


def solution(mesh):
    in_specs = (P("tok", "exp"), P("exp", None), P("tok", None), P("exp"))
    out_specs = (P("tok", "exp"), P("tok", None), P(), P())
    return jax.shard_map(functools.partial(local, mesh.shape["tok"]), mesh=mesh,
                         in_specs=in_specs, out_specs=out_specs, check_vma=False)
```

```python
import functools

import jax
import jax.numpy as jnp
from jax import lax
from jax.experimental import pallas as pl
from jax.experimental.pallas import tpu as pltpu
from jax.sharding import PartitionSpec as P

MESH = pl.DeviceIdType.MESH
F32 = jnp.float32
LINK = jnp.int16
TOP_CODE = 32760.0
TOKEN_BOUND, GATE_BOUND = 6.0, 0.0625
W_CHUNKS = 4
RAW_AT = (0, 2)
LAG = (3, 5)
HELD = 4
AHEAD = 4
ROOT = 1


def plan(n):
    turn = list(range(1, n))
    turn.insert(min(3, n - 1), 0)
    order = []
    for j in range(n + max(LAG)):
        if j <= n:
            order.append(("a", j))
        order += [(core, turn[j - LAG[core]]) for core in (0, 1) if 0 <= j - LAG[core] < n]
    return order


def kernel(ntok, widths, x_hbm, w_hbm, ids_hbm, bias_hbm,
           affv, wtsv, load_ref, newb_ref,
           xv, wv, ids, bias_all, part, rx1, keep, mine, tx2, rx2, tx3, rx3, cnt, fin,
           l_sem, s1, r1, s2, r2, s3, r3, sc, rc, rb, ready):
    half = widths[0] // 2
    units = [(sum(widths[:i]), widths[i], i) for i in range(1, len(widths))]
    for k, place in enumerate(RAW_AT):
        units.insert(place, (k * half, half, 0))
    sizes = sorted({width for _, width, _ in units})
    acc_of = [2 * sizes.index(width) + sum(w == width for _, w, _ in units[:j]) % 2
              for j, (_, width, _) in enumerate(units)]
    specs = [tuple(pltpu.ACC(q)((width, 256), F32) for q in (0, 1)) for width in sizes for _ in range(2)]
    pl.run_scoped(functools.partial(body, ntok, widths, units, acc_of, (
        x_hbm, w_hbm, ids_hbm, bias_hbm, affv, wtsv, load_ref, newb_ref,
        xv, wv, ids, bias_all, part, rx1, keep, mine, tx2, rx2, tx3, rx3, cnt, fin,
        l_sem, s1, r1, s2, r2, s3, r3, sc, rc, rb, ready)), *specs)


def body(ntok, widths, units, acc_of, refs, *accs):
    (x_hbm, w_hbm, ids_hbm, bias_hbm, affv, wtsv, load_ref, newb_ref,
     xv, wv, ids, bias_all, part, rx1, keep, mine, tx2, rx2, tx3, rx3, cnt, fin,
     l_sem, s1, r1, s2, r2, s3, r3, sc, rc, rb, ready) = refs
    own = bias_all.shape[2]
    top, rows = ids.shape
    depth = xv.shape[1]
    n = len(widths)
    starts = [sum(widths[:i]) for i in range(n)]
    t, e = lax.axis_index("tok"), lax.axis_index("exp")
    y, c = e // 2, e % 2
    mate = 2 * y + 1 - c
    peer = 2 * (1 - y) + c
    cross = 2 * (1 - y) + 1 - c
    experts = 4 * own
    is_root = e == ROOT
    others = [k for k in range(4) if k != ROOT]

    def cols(i):
        return pl.ds(starts[i], widths[i])

    nu = len(units)

    def unit(j):
        return pl.ds(*units[j][:2])

    chunk = -(-depth // W_CHUNKS // 256) * 256
    chunks = [pl.ds(k, min(chunk, depth - k)) for k in range(0, depth, chunk)]
    w_in = [pltpu.make_async_copy(w_hbm.at[k], wv.at[k], l_sem.at[0]) for k in chunks]
    w_all = pltpu.make_async_copy(w_hbm, wv, l_sem.at[0])
    ids_in = pltpu.make_async_copy(ids_hbm, ids, l_sem.at[1])
    slot = [2 + i if i < AHEAD else 0 if i == AHEAD else 2 + (i - AHEAD - 1) % AHEAD for i in range(nu)]
    x_in = [pltpu.make_async_copy(x_hbm.at[unit(j)], xv.at[unit(j)], l_sem.at[slot[j]]) for j in range(nu)]
    ids_in.start()
    for copy in w_in + x_in[:AHEAD]:
        copy.start()

    barrier = pltpu.get_barrier_semaphore()

    for k in others:
        @pl.when(e != k)
        def _():
            pl.semaphore_signal(barrier, inc=1, device_id=(t, k), device_id_type=MESH)

    bias_in = pltpu.make_async_copy(bias_hbm, bias_all.at[ROOT], sc)
    bias_out = pltpu.make_async_remote_copy(
        src_ref=bias_hbm, dst_ref=bias_all.at[e], send_sem=sc, recv_sem=rb,
        device_id=(t, ROOT), device_id_type=MESH)
    bias_back = pltpu.make_async_remote_copy(
        src_ref=bias_all.at[pl.ds(0, 3)], dst_ref=bias_all.at[pl.ds(0, 3)], send_sem=sc, recv_sem=rb,
        device_id=(t, mate), device_id_type=MESH)
    cnt_out = [pltpu.make_async_remote_copy(
        src_ref=cnt.at[0], dst_ref=cnt.at[d], send_sem=sc, recv_sem=rc,
        device_id=((t + d) % ntok, e), device_id_type=MESH) for d in range(1, ntok)]
    rest = pl.ds(1, ntok - 1)
    cnt_all = pltpu.make_async_remote_copy(
        src_ref=cnt.at[rest], dst_ref=cnt.at[rest], send_sem=sc, recv_sem=rc,
        device_id=(t, mate), device_id_type=MESH)
    fin_out = [pltpu.make_async_remote_copy(
        src_ref=fin.at[j], dst_ref=fin.at[3], send_sem=sc, recv_sem=rc,
        device_id=(t, k), device_id_type=MESH) for j, k in enumerate(others)]
    fin_all = pltpu.make_async_remote_copy(
        src_ref=fin.at[pl.ds(0, 3)], dst_ref=fin.at[pl.ds(0, 3)], send_sem=sc, recv_sem=rc,
        device_id=(t, mate), device_id_type=MESH)

    @pl.when(is_root)
    def _():
        bias_in.start()
        for d in range(1, ntok):
            pl.semaphore_signal(barrier, inc=1, device_id=((t + d) % ntok, e), device_id_type=MESH)
        ids_in.wait()
        lanes = 128
        numbers = lax.broadcasted_iota(jnp.int32, (experts, lanes), 0).astype(F32).astype(jnp.bfloat16)
        one, zero = jnp.bfloat16(1), jnp.bfloat16(0)
        exact = 256 // top
        blocks = rows // lanes
        total = jnp.zeros((1, experts), F32)
        for g0 in range(0, blocks, exact):
            acc = jnp.zeros((experts, lanes), jnp.bfloat16)
            for g in range(g0, min(g0 + exact, blocks)):
                found = ids[:, pl.ds(g * lanes, lanes)].astype(F32).astype(jnp.bfloat16)
                for j in range(top):
                    acc = acc + jnp.where(found[j:j + 1] == numbers, one, zero)
            total = total + jnp.sum(acc.astype(F32).T, axis=0, keepdims=True)
        cnt[0] = total.astype(jnp.int32)
        bias_in.wait()

    @pl.when(jnp.logical_not(is_root))
    def _():
        pl.semaphore_wait(barrier, 3)
        pl.semaphore_signal(ready, inc=1, device_id=(t, ROOT), device_id_type=MESH)
        bias_out.start()
        ids_in.wait()

    queue = list(range(AHEAD, nu))

    def more_tokens(freed):
        if queue and slot[queue[0]] == freed:
            x_in[queue.pop(0)].start()

    def send_counts():
        pl.semaphore_wait(barrier, ntok - 1)
        for copy in cnt_out:
            copy.start()

    def send_counts_soon():
        pl.when(jnp.logical_and(is_root, 2 * t >= ntok))(send_counts)

    def send_counts_late():
        pl.when(jnp.logical_and(is_root, 2 * t < ntok))(send_counts)

    def finish_counts():
        @pl.when(is_root)
        def _():
            cnt_all.wait()
            bias_back.wait_recv()
            total = cnt[0]
            for d in range(1, ntok):
                total = total + cnt[d]
            load = total.astype(F32)
            target = F32(ntok * rows * top)
            gap = target - F32(experts) * load
            sign = jnp.where(gap > 0, F32(1), jnp.where(gap < 0, F32(-1), F32(0)))
            bias = jnp.concatenate([bias_all[k] for k in range(4)], axis=1)
            for j in range(4):
                fin[j, 0] = load
                fin[j, 1] = bias + 0.001 * sign
            for copy in fin_out:
                copy.start()

    def close_counts():
        @pl.when(is_root)
        def _():
            fin_all.wait_send()

        @pl.when(jnp.logical_not(is_root))
        def _():
            fin_out[0].wait_recv()
            bias_out.wait_send()

        load_ref[...] = fin[3, 0]
        newb_ref[...] = fin[3, 1]

    def first(at, i):
        return pltpu.make_async_remote_copy(
            src_ref=part.at[1 - c, :, at], dst_ref=rx1.at[:, at],
            send_sem=s1, recv_sem=r1.at[i], device_id=(t, mate), device_id_type=MESH)

    def second(at, i):
        return pltpu.make_async_remote_copy(
            src_ref=tx2.at[:, at], dst_ref=rx2.at[:, at],
            send_sem=s2, recv_sem=r2.at[i], device_id=(t, peer), device_id_type=MESH)

    def across(j):
        at = pl.ds(rows + units[j][0], units[j][1])
        return pltpu.make_async_remote_copy(
            src_ref=tx2.at[:, at], dst_ref=rx2.at[:, at],
            send_sem=s2, recv_sem=r2.at[0], device_id=(t, cross), device_id_type=MESH)

    chosen_out = pltpu.make_async_remote_copy(
        src_ref=tx3, dst_ref=rx3, send_sem=s3, recv_sem=r3, device_id=(t, peer), device_id_type=MESH)
    hand_on = pltpu.make_async_remote_copy(
        src_ref=rx3, dst_ref=rx3, send_sem=s3, recv_sem=r3, device_id=(t, mate), device_id_type=MESH)

    side = 256
    tiles = depth // side
    shares = [[(q, k) for q in (0, 1) for k in range(tiles)
               if (k < (tiles + 1 - i % 2) // 2) == (q == 0)] for i in range(nu)]
    line = [[(i, k) for i in range(nu) for p, k in shares[i] if p == q] for q in (0, 1)]
    where = [0, 0]

    def push(q):
        if where[q] < len(line[q]):
            k = line[q][where[q]][1]
            pltpu.matmul_push_rhs(wv[pl.ds(k * side, side), :], staging_register=where[q] % 2, mxu_index=q)

    def issue(i):
        x_in[i].wait()
        more_tokens(slot[i])
        left = [[k for p, k in shares[i] if p == q] for q in (0, 1)]
        for step in range(max(map(len, left))):
            for q in (0, 1):
                if step < len(left[q]):
                    k = left[q][step]
                    mark = where[q] % 2
                    where[q] += 1
                    push(q)
                    pltpu.matmul_acc_lhs(accs[acc_of[i]][q], xv[unit(i), pl.ds(k * side, side)], load_staged_rhs=mark)

    def product(j):
        at = unit(j)
        if j + 1 < nu:
            issue(j + 1)
        r = (pltpu.matmul_pop(accs[acc_of[j]][0]) + pltpu.matmul_pop(accs[acc_of[j]][1])).T
        for k in range(4):
            part[k % 2, pl.ds(k // 2 * own, own), at] = r[k * own:(k + 1) * own]

    def pick(at):
        mine_ids = ids[:, at]
        low, high = mine_ids & 7, mine_ids >> 3
        picked = jnp.zeros(mine_ids.shape, F32)
        for k in range(experts // 8):
            block, line = divmod(8 * k, own)
            rows8 = part[block % 2, pl.ds(block // 2 * own + line, 8), at]
            row = jnp.take_along_axis(rows8, low, axis=0, mode="promise_in_bounds")
            picked = jnp.where(high == k, row, picked)
        for k in range(2):
            part[k, pl.ds(2 * own, top), at] = picked

    def to_mate(i):
        pick(cols(i))
        first(cols(i), i).start()

    def stage_a(j):
        product(j)
        if j == 0:
            @pl.when(is_root)
            def _():
                pl.semaphore_wait(ready, 3)
        start, width, i = units[j]
        if i == 0:
            tx2[:, unit(j)] = encode(part[c, theirs, unit(j)]).astype(LINK)
            tx2[:, pl.ds(rows + start, width)] = encode(part[1 - c, theirs, unit(j)]).astype(LINK)
            second(unit(j), 0).start()
            across(j).start()
        else:
            to_mate(i)
        if j == RAW_AT[-1] + 1:
            to_mate(0)

    bound = 2 * depth * TOKEN_BOUND * GATE_BOUND
    grain = TOP_CODE / bound ** 0.25

    def encode(v):
        size = lax.rsqrt(lax.rsqrt(jnp.abs(v) + F32(1e-30))) * F32(grain) + F32(0.5)
        return jnp.where(v < 0, -size, size).astype(jnp.int32)

    def decode(whole):
        u = whole.astype(F32)
        return (u * u * F32(grain ** -4)) * (u * jnp.abs(u))

    theirs = pl.ds(pl.multiple_of((1 - y) * own, own), own)
    ours = pl.ds(pl.multiple_of(y * own, own), own)
    picks = pl.ds(2 * own, top)

    def stage_b(i, core):
        first(cols(i), i).wait_recv()
        if i > 0:
            tx2[:, cols(i)] = encode(part[c, theirs, cols(i)] + rx1[theirs, cols(i)]).astype(LINK)
            if core == 0 or i < n - HELD:
                second(cols(i), i).start()
        chosen = encode(part[c, picks, cols(i)] + rx1[picks, cols(i)])
        if core == 1:
            tx3[:, cols(i)] = chosen.astype(LINK)
        if core == 1 and i == n - 1:
            chosen_out.start()
            for k in range(n - HELD, n):
                second(cols(k), k).start()
        keep[:, cols(i)] = part[c, ours, cols(i)] + rx1[ours, cols(i)]
        mine[:, cols(i)] = decode(chosen)

    def weigh():
        chosen = 1.0 / (1.0 + jnp.exp(-(mine[...] + decode(rx3[...].astype(jnp.int32)))))
        wtsv[...] = 2.5 * chosen / jnp.sum(chosen, axis=0, keepdims=True)

    def stage_c(i):
        second(pl.ds(0, 2 * widths[0]) if i == 0 else cols(i), i).wait_recv()
        logits = keep[:, cols(i)] + decode(rx2[:, cols(i)].astype(jnp.int32))
        if i == 0:
            logits = logits + decode(rx2[:, pl.ds(rows, widths[0])].astype(jnp.int32))
        affv[:, cols(i)] = 1.0 / (1.0 + jnp.exp(-logits))

    w_all.wait()
    more_tokens(0)
    for q in (0, 1):
        push(q)
    issue(0)
    for kind, i in plan(n):
        if kind == "a":
            stage_a(i)
        else:
            pl.when(c == kind)(functools.partial(stage_b, i, kind))
        if (kind, i) == ("a", 1):
            send_counts_soon()
        if (kind, i) == ("a", n):
            send_counts_late()
    for i in range(n):
        if i == n - HELD:
            @pl.when(c == 1)
            def _():
                chosen_out.wait()
                hand_on.start()
            finish_counts()
        if i == n - 1:
            pl.when(c == 0)(hand_on.wait_recv)
            weigh()
        stage_c(i)
    close_counts()
    first(pl.ds(0, rows), 0).wait_send()
    second(pl.ds(0, rows + widths[0]), 0).wait_send()
    pl.when(c == 1)(hand_on.wait_send)


def place(aff, wts, load, newb, aff_hbm, wts_hbm, load_hbm, newb_hbm, sem):
    copies = [pltpu.make_async_copy(a, b, sem.at[k]) for k, (a, b) in enumerate(
        ((aff, aff_hbm), (wts, wts_hbm), (load, load_hbm), (newb, newb_hbm)))]
    for copy in copies:
        copy.start()
    for copy in copies:
        copy.wait()


def local(ntok, tokens, gate_weight, expert_ids, expert_bias):
    rows, depth = tokens.shape
    experts = gate_weight.shape[1]
    own = expert_bias.shape[0]
    top = expert_ids.shape[1]
    piece = 256
    widths = [piece] * (rows // piece)
    n = len(widths)
    dma = pltpu.SemaphoreType.DMA
    vm = pltpu.VMEM
    any_ = pl.BlockSpec(memory_space=pl.ANY)
    vmem = pl.BlockSpec(memory_space=pltpu.VMEM)
    shapes = ((own, rows), (top, rows), (1, experts), (1, experts))
    results = pl.pallas_call(
        functools.partial(kernel, ntok, widths),
        out_shape=tuple(pltpu.VMEM(shape, F32) for shape in shapes),
        in_specs=[any_] * 4,
        out_specs=(vmem,) * 4,
        scratch_shapes=[
            vm((rows, depth), tokens.dtype), vm((depth, experts), gate_weight.dtype),
            vm((top, rows), jnp.int32),
            vm((4, 1, own), F32),
            vm((2, 2 * own + top, rows), F32), vm((2 * own + top, rows), F32),
            vm((own, rows), F32), vm((top, rows), F32),
            vm((own, rows + piece), LINK), vm((own, rows + piece), LINK),
            vm((top, rows), LINK), vm((top, rows), LINK),
            vm((ntok, 1, experts), jnp.int32), vm((4, 2, 1, experts), F32),
            dma((2 + AHEAD,)), dma, dma((n,)), dma, dma((n,)), dma, dma, dma, dma, dma,
            pltpu.SemaphoreType.REGULAR,
        ],
        compiler_params=pltpu.CompilerParams(
            collective_id=0, has_side_effects=True, vmem_limit_bytes=60 * 1024 * 1024),
    )(tokens, gate_weight, expert_ids.T, expert_bias.reshape(1, own))
    aff, wts, load, newb = pl.pallas_call(
        place,
        out_shape=tuple(jax.ShapeDtypeStruct(shape, F32) for shape in shapes),
        in_specs=[vmem] * 4,
        out_specs=(pl.BlockSpec(memory_space=pltpu.HBM),) * 4,
        scratch_shapes=[dma((4,))],
    )(*(pltpu.with_memory_space_constraint(r, pltpu.VMEM) for r in results))
    return aff.T, wts.T, load.reshape(experts), newb.reshape(experts)


def solution(mesh):
    in_specs = (P("tok", "exp"), P("exp", None), P("tok", None), P("exp"))
    out_specs = (P("tok", "exp"), P("tok", None), P(), P())
    return jax.shard_map(functools.partial(local, mesh.shape["tok"]), mesh=mesh,
                         in_specs=in_specs, out_specs=out_specs, check_vma=False)
```

```python
import functools
import math

import jax
import jax.numpy as jnp
from jax import lax
from jax.experimental import pallas as pl
from jax.experimental.pallas import tpu as pltpu
from jax.sharding import PartitionSpec as P

MESH = pl.DeviceIdType.MESH
F32 = jnp.float32
LINK = jnp.int16
TOP_CODE = 32760.0
TOKEN_BOUND, GATE_BOUND = 6.0, 0.0625
W_CHUNKS = 4
RAW_AT = (0, 2)
MATE_RUNS = (1, 1, 2, 1, 1, 2)
PEER_RUNS = (1, 3, 2, 1, 1)
LAG = (3, 5)
HELD = 4
AHEAD = 4
ROOT = 1


def grouped(items, sizes):
    runs, at = [], 0
    for size in list(sizes) + [1] * len(items):
        if at < len(items):
            runs.append(items[at:at + size])
            at += size
    return runs


def turns(n):
    turn = list(range(1, n))
    turn.insert(min(3, n - 1), 0)
    return turn


def plan(n):
    turn = turns(n)
    order = []
    for j in range(n + max(LAG)):
        if j <= n:
            order.append(("a", j))
        order += [(core, turn[j - LAG[core]]) for core in (0, 1) if 0 <= j - LAG[core] < n]
    return order


def kernel(ntok, widths, x_hbm, w_hbm, ids_hbm, bias_hbm,
           wide, thin,
           xv, wv, ids, bias_all, part, rx1, keep, mine, tx2, rx2, tx3, rx3, cnt, fin,
           l_sem, s1, r1, s2, r2, s3, r3, sc, rc, rb, ready):
    half = widths[0] // 2
    units = [(sum(widths[:i]), widths[i], i) for i in range(1, len(widths))]
    for k, place in enumerate(RAW_AT):
        units.insert(place, (k * half, half, 0))
    sizes = sorted({width for _, width, _ in units})
    acc_of = [2 * sizes.index(width) + sum(w == width for _, w, _ in units[:j]) % 2
              for j, (_, width, _) in enumerate(units)]
    specs = [tuple(pltpu.ACC(q)((width, 256), F32) for q in (0, 1)) for width in sizes for _ in range(2)]
    pl.run_scoped(functools.partial(body, ntok, widths, units, acc_of, (
        x_hbm, w_hbm, ids_hbm, bias_hbm, wide, thin,
        xv, wv, ids, bias_all, part, rx1, keep, mine, tx2, rx2, tx3, rx3, cnt, fin,
        l_sem, s1, r1, s2, r2, s3, r3, sc, rc, rb, ready)), *specs)


def body(ntok, widths, units, acc_of, refs, *accs):
    (x_hbm, w_hbm, ids_hbm, bias_hbm, wide, thin,
     xv, wv, ids, bias_all, part, rx1, keep, mine, tx2, rx2, tx3, rx3, cnt, fin,
     l_sem, s1, r1, s2, r2, s3, r3, sc, rc, rb, ready) = refs
    own = bias_all.shape[2]
    top, rows = ids.shape
    depth = xv.shape[1]
    n = len(widths)
    starts = [sum(widths[:i]) for i in range(n)]
    t, e = lax.axis_index("tok"), lax.axis_index("exp")
    y, c = e // 2, e % 2
    mate = 2 * y + 1 - c
    peer = 2 * (1 - y) + c
    cross = 2 * (1 - y) + 1 - c
    experts = 4 * own
    is_root = e == ROOT
    others = [k for k in range(4) if k != ROOT]

    def cols(i):
        return pl.ds(starts[i], widths[i])

    nu = len(units)
    mate_runs, peer_runs = grouped(turns(n), MATE_RUNS), grouped(list(range(n)), PEER_RUNS)
    mate_run = {i: k for k, run in enumerate(mate_runs) for i in run}
    peer_run = {i: k for k, run in enumerate(peer_runs) for i in run}

    def unit(j):
        return pl.ds(*units[j][:2])

    def within(j):
        start, width, i = units[j]
        return pl.ds(start - starts[i], width)

    chunk = -(-depth // W_CHUNKS // 256) * 256
    chunks = [pl.ds(k, min(chunk, depth - k)) for k in range(0, depth, chunk)]
    w_in = [pltpu.make_async_copy(w_hbm.at[k], wv.at[k], l_sem.at[0]) for k in chunks]
    w_all = pltpu.make_async_copy(w_hbm, wv, l_sem.at[0])
    ids_in = pltpu.make_async_copy(ids_hbm, ids, l_sem.at[1])
    slot = [2 + i if i < AHEAD else 0 if i == AHEAD else 2 + (i - AHEAD - 1) % AHEAD for i in range(nu)]
    x_in = [pltpu.make_async_copy(x_hbm.at[unit(j)], xv.at[unit(j)], l_sem.at[slot[j]]) for j in range(nu)]
    ids_in.start()
    for copy in w_in + x_in[:AHEAD]:
        copy.start()

    barrier = pltpu.get_barrier_semaphore()

    for k in others:
        @pl.when(e != k)
        def _():
            pl.semaphore_signal(barrier, inc=1, device_id=(t, k), device_id_type=MESH)

    bias_in = pltpu.make_async_copy(bias_hbm, bias_all.at[ROOT], sc)
    bias_out = pltpu.make_async_remote_copy(
        src_ref=bias_hbm, dst_ref=bias_all.at[e], send_sem=sc, recv_sem=rb,
        device_id=(t, ROOT), device_id_type=MESH)
    bias_back = pltpu.make_async_remote_copy(
        src_ref=bias_all.at[pl.ds(0, 3)], dst_ref=bias_all.at[pl.ds(0, 3)], send_sem=sc, recv_sem=rb,
        device_id=(t, mate), device_id_type=MESH)
    cnt_out = [pltpu.make_async_remote_copy(
        src_ref=cnt.at[0], dst_ref=cnt.at[d], send_sem=sc, recv_sem=rc,
        device_id=((t + d) % ntok, e), device_id_type=MESH) for d in range(1, ntok)]
    rest = pl.ds(1, ntok - 1)
    cnt_all = pltpu.make_async_remote_copy(
        src_ref=cnt.at[rest], dst_ref=cnt.at[rest], send_sem=sc, recv_sem=rc,
        device_id=(t, mate), device_id_type=MESH)
    fin_out = [pltpu.make_async_remote_copy(
        src_ref=fin.at[j], dst_ref=fin.at[3], send_sem=sc, recv_sem=rc,
        device_id=(t, k), device_id_type=MESH) for j, k in enumerate(others)]
    fin_all = pltpu.make_async_remote_copy(
        src_ref=fin.at[pl.ds(0, 3)], dst_ref=fin.at[pl.ds(0, 3)], send_sem=sc, recv_sem=rc,
        device_id=(t, mate), device_id_type=MESH)

    @pl.when(is_root)
    def _():
        bias_in.start()
        for d in range(1, ntok):
            pl.semaphore_signal(barrier, inc=1, device_id=((t + d) % ntok, e), device_id_type=MESH)
        ids_in.wait()
        lanes = 128
        numbers = lax.broadcasted_iota(jnp.int32, (experts, lanes), 0).astype(F32).astype(jnp.bfloat16)
        one, zero = jnp.bfloat16(1), jnp.bfloat16(0)
        exact = 256 // top
        blocks = rows // lanes
        total = jnp.zeros((1, experts), F32)
        for g0 in range(0, blocks, exact):
            acc = jnp.zeros((experts, lanes), jnp.bfloat16)
            for g in range(g0, min(g0 + exact, blocks)):
                found = ids[:, pl.ds(g * lanes, lanes)].astype(F32).astype(jnp.bfloat16)
                for j in range(top):
                    acc = acc + jnp.where(found[j:j + 1] == numbers, one, zero)
            total = total + jnp.sum(acc.astype(F32).T, axis=0, keepdims=True)
        cnt[0] = total.astype(jnp.int32)
        bias_in.wait()

    @pl.when(jnp.logical_not(is_root))
    def _():
        pl.semaphore_wait(barrier, 3)
        pl.semaphore_signal(ready, inc=1, device_id=(t, ROOT), device_id_type=MESH)
        bias_out.start()
        ids_in.wait()

    queue = list(range(AHEAD, nu))

    def more_tokens(freed):
        if queue and slot[queue[0]] == freed:
            x_in[queue.pop(0)].start()

    def send_counts():
        pl.semaphore_wait(barrier, ntok - 1)
        for copy in cnt_out:
            copy.start()

    def send_counts_soon():
        pl.when(jnp.logical_and(is_root, 2 * t >= ntok))(send_counts)

    def send_counts_late():
        pl.when(jnp.logical_and(is_root, 2 * t < ntok))(send_counts)

    def finish_counts():
        @pl.when(is_root)
        def _():
            cnt_all.wait()
            bias_back.wait_recv()
            total = cnt[0]
            for d in range(1, ntok):
                total = total + cnt[d]
            load = total.astype(F32)
            target = F32(ntok * rows * top)
            gap = target - F32(experts) * load
            sign = jnp.where(gap > 0, F32(1), jnp.where(gap < 0, F32(-1), F32(0)))
            bias = jnp.concatenate([bias_all[k] for k in range(4)], axis=1)
            for j in range(4):
                fin[j, 0] = load
                fin[j, 1] = bias + 0.001 * sign
            for copy in fin_out:
                copy.start()

    def close_counts():
        @pl.when(is_root)
        def _():
            fin_all.wait_send()

        @pl.when(jnp.logical_not(is_root))
        def _():
            fin_out[0].wait_recv()
            bias_out.wait_send()

        thin[...] = fin[3]

    def first(at, k):
        return pltpu.make_async_remote_copy(
            src_ref=part.at[1 - c, at], dst_ref=rx1.at[at],
            send_sem=s1, recv_sem=r1.at[k], device_id=(t, mate), device_id_type=MESH)

    def second(at, k):
        return pltpu.make_async_remote_copy(
            src_ref=tx2.at[at], dst_ref=rx2.at[at],
            send_sem=s2, recv_sem=r2.at[k], device_id=(t, peer), device_id_type=MESH)

    def raw(j):
        return pltpu.make_async_remote_copy(
            src_ref=tx2.at[0, :, within(j)], dst_ref=rx2.at[0, :, within(j)],
            send_sem=s2, recv_sem=r2.at[0], device_id=(t, peer), device_id_type=MESH)

    def across(j):
        return pltpu.make_async_remote_copy(
            src_ref=tx2.at[n, :, within(j)], dst_ref=rx2.at[n, :, within(j)],
            send_sem=s2, recv_sem=r2.at[0], device_id=(t, cross), device_id_type=MESH)

    chosen_out = pltpu.make_async_remote_copy(
        src_ref=tx3, dst_ref=rx3, send_sem=s3, recv_sem=r3, device_id=(t, peer), device_id_type=MESH)
    hand_on = pltpu.make_async_remote_copy(
        src_ref=rx3, dst_ref=rx3, send_sem=s3, recv_sem=r3, device_id=(t, mate), device_id_type=MESH)

    def arrival(i, runs, copy, blocks):
        for k, run in enumerate(runs):
            if run[0] == i:
                copy(pl.ds(0, sum(blocks(m) for m in run)), k).wait_recv()

    side = 256
    tiles = depth // side
    shares = [[(q, k) for q in (0, 1) for k in range(tiles)
               if (k < (tiles + 1 - i % 2) // 2) == (q == 0)] for i in range(nu)]
    line = [[(i, k) for i in range(nu) for p, k in shares[i] if p == q] for q in (0, 1)]
    where = [0, 0]

    def push(q):
        if where[q] < len(line[q]):
            k = line[q][where[q]][1]
            pltpu.matmul_push_rhs(wv[pl.ds(k * side, side), :], staging_register=where[q] % 2, mxu_index=q)

    def issue(i):
        x_in[i].wait()
        more_tokens(slot[i])
        left = [[k for p, k in shares[i] if p == q] for q in (0, 1)]
        for step in range(max(map(len, left))):
            for q in (0, 1):
                if step < len(left[q]):
                    k = left[q][step]
                    mark = where[q] % 2
                    where[q] += 1
                    push(q)
                    pltpu.matmul_acc_lhs(accs[acc_of[i]][q], xv[unit(i), pl.ds(k * side, side)], load_staged_rhs=mark)

    def product(j):
        if 0 < j < nu - 1:
            issue(j + 1)
        r = (pltpu.matmul_pop(accs[acc_of[j]][0]) + pltpu.matmul_pop(accs[acc_of[j]][1])).T
        for k in range(4):
            part[k % 2, units[j][2], pl.ds(k // 2 * own, own), within(j)] = r[k * own:(k + 1) * own]

    def pick(i):
        mine_ids = ids[:, cols(i)]
        low, high = mine_ids & 7, mine_ids >> 3
        picked = jnp.zeros(mine_ids.shape, F32)
        for k in range(experts // 8):
            block, line = divmod(8 * k, own)
            rows8 = part[block % 2, i, pl.ds(block // 2 * own + line, 8), :]
            row = jnp.take_along_axis(rows8, low, axis=0, mode="promise_in_bounds")
            picked = jnp.where(high == k, row, picked)
        for k in range(2):
            part[k, i, pl.ds(2 * own, top), :] = picked

    def to_mate(i):
        pick(i)
        first(i, mate_run[i]).start()

    def stage_a(j):
        product(j)
        if j == 0:
            @pl.when(is_root)
            def _():
                pl.semaphore_wait(ready, 3)
        start, width, i = units[j]
        if i == 0:
            tx2[0, :, within(j)] = encode(part[c, 0, theirs, within(j)]).astype(LINK)
            tx2[n, :, within(j)] = encode(part[1 - c, 0, theirs, within(j)]).astype(LINK)
            raw(j).start()
            across(j).start()
        else:
            to_mate(i)
        if j == 0:
            issue(1)
        if j == RAW_AT[-1] + 1:
            to_mate(0)

    bound = 2 * depth * TOKEN_BOUND * GATE_BOUND
    grain = TOP_CODE / math.asinh(bound)

    def encode(v):
        size = jnp.abs(v)
        code = jnp.log(size + jnp.sqrt(size * size + F32(1))) * F32(grain) + F32(0.5)
        return jnp.where(v < 0, -code, code).astype(jnp.int32)

    def decode(whole):
        grown = jnp.exp(whole.astype(F32) * F32(1 / grain))
        return F32(0.5) * grown - F32(0.5) / grown

    theirs = pl.ds(pl.multiple_of((1 - y) * own, own), own)
    ours = pl.ds(pl.multiple_of(y * own, own), own)
    picks = pl.ds(2 * own, top)

    def stage_b(i, core):
        arrival(i, mate_runs, first, lambda m: 1)
        if i > 0:
            tx2[i] = encode(part[c, i, theirs] + rx1[i, theirs]).astype(LINK)
            if core == 0 or i < n - HELD:
                second(i, peer_run[i]).start()
        chosen = encode(part[c, i, picks] + rx1[i, picks])
        if core == 1:
            tx3[:, cols(i)] = chosen.astype(LINK)
        if core == 1 and i == n - 1:
            chosen_out.start()
            for k in range(n - HELD, n):
                second(k, peer_run[k]).start()
        keep[:, cols(i)] = part[c, i, ours] + rx1[i, ours]
        mine[:, cols(i)] = decode(chosen)

    def weigh():
        chosen = 1.0 / (1.0 + jnp.exp(-(mine[...] + decode(rx3[...].astype(jnp.int32)))))
        wide[own:] = 2.5 * chosen / jnp.sum(chosen, axis=0, keepdims=True)

    def stage_c(i):
        arrival(i, peer_runs, second, lambda m: 2 if m == 0 else 1)
        logits = keep[:, cols(i)] + decode(rx2[i].astype(jnp.int32))
        if i == 0:
            logits = logits + decode(rx2[n].astype(jnp.int32))
        wide[0:own, cols(i)] = 1.0 / (1.0 + jnp.exp(-logits))

    w_all.wait()
    more_tokens(0)
    for q in (0, 1):
        push(q)
    issue(0)
    for kind, i in plan(n):
        if kind == "a":
            stage_a(i)
        else:
            pl.when(c == kind)(functools.partial(stage_b, i, kind))
        if (kind, i) == ("a", 1):
            send_counts_soon()
        if (kind, i) == ("a", n):
            send_counts_late()
    for i in range(n):
        if i == n - HELD:
            @pl.when(c == 1)
            def _():
                chosen_out.wait()
                hand_on.start()
            finish_counts()
        if i == n - 1:
            pl.when(c == 0)(hand_on.wait_recv)
            weigh()
        stage_c(i)
    close_counts()
    first(pl.ds(0, n), 0).wait_send()
    second(pl.ds(0, n + 1), 0).wait_send()
    pl.when(c == 1)(hand_on.wait_send)


def place(wide, thin, aff_hbm, wts_hbm, load_hbm, newb_hbm, sem):
    for k, (source, results) in enumerate(((wide, (aff_hbm, wts_hbm)), (thin, (load_hbm, newb_hbm)))):
        at = 0
        for result in results:
            pltpu.make_async_copy(source.at[pl.ds(at, result.shape[0])], result, sem.at[k]).start()
            at += result.shape[0]
    for k, source in enumerate((wide, thin)):
        pltpu.make_async_copy(source, source, sem.at[k]).wait()


def local(ntok, tokens, gate_weight, expert_ids, expert_bias):
    rows, depth = tokens.shape
    experts = gate_weight.shape[1]
    own = expert_bias.shape[0]
    top = expert_ids.shape[1]
    piece = 256
    widths = [piece] * (rows // piece)
    n = len(widths)
    dma = pltpu.SemaphoreType.DMA
    vm = pltpu.VMEM
    any_ = pl.BlockSpec(memory_space=pl.ANY)
    vmem = pl.BlockSpec(memory_space=pltpu.VMEM)
    shapes = ((own, rows), (top, rows), (1, 1, experts), (1, 1, experts))
    results = pl.pallas_call(
        functools.partial(kernel, ntok, widths),
        out_shape=(pltpu.VMEM((own + top, rows), F32), pltpu.VMEM((2, 1, experts), F32)),
        in_specs=[any_] * 4,
        out_specs=(vmem,) * 2,
        scratch_shapes=[
            vm((rows, depth), tokens.dtype), vm((depth, experts), gate_weight.dtype),
            vm((top, rows), jnp.int32),
            vm((4, 1, own), F32),
            vm((2, n, 2 * own + top, piece), F32), vm((n, 2 * own + top, piece), F32),
            vm((own, rows), F32), vm((top, rows), F32),
            vm((n + 1, own, piece), LINK), vm((n + 1, own, piece), LINK),
            vm((top, rows), LINK), vm((top, rows), LINK),
            vm((ntok, 1, experts), jnp.int32), vm((4, 2, 1, experts), F32),
            dma((2 + AHEAD,)), dma, dma((len(grouped(turns(n), MATE_RUNS)),)),
            dma, dma((len(grouped(turns(n), PEER_RUNS)),)), dma, dma, dma, dma, dma,
            pltpu.SemaphoreType.REGULAR,
        ],
        compiler_params=pltpu.CompilerParams(
            collective_id=0, has_side_effects=True, vmem_limit_bytes=60 * 1024 * 1024),
    )(tokens, gate_weight, expert_ids.T, expert_bias.reshape(1, own))
    aff, wts, load, newb = pl.pallas_call(
        place,
        out_shape=tuple(jax.ShapeDtypeStruct(shape, F32) for shape in shapes),
        in_specs=[vmem] * 2,
        out_specs=(pl.BlockSpec(memory_space=pltpu.HBM),) * 4,
        scratch_shapes=[dma((2,))],
    )(*(pltpu.with_memory_space_constraint(r, pltpu.VMEM) for r in results))
    return aff.T, wts.T, load.reshape(experts), newb.reshape(experts)


def solution(mesh):
    in_specs = (P("tok", "exp"), P("exp", None), P("tok", None), P("exp"))
    out_specs = (P("tok", "exp"), P("tok", None), P(), P())
    return jax.shard_map(functools.partial(local, mesh.shape["tok"]), mesh=mesh,
                         in_specs=in_specs, out_specs=out_specs, check_vma=False)
```

```python
import functools
import math

import jax
import jax.numpy as jnp
from jax import lax
from jax.experimental import pallas as pl
from jax.experimental.pallas import tpu as pltpu
from jax.sharding import PartitionSpec as P

MESH = pl.DeviceIdType.MESH
F32 = jnp.float32
LINK = jnp.int16
TOP_CODE = 32760.0
TOKEN_BOUND, GATE_BOUND = 6.0, 0.0625
W_CHUNKS = 4
RAW_AT = (0, 2)
MATE_RUNS = (1, 1, 1, 2, 1, 2)
PEER_RUNS = (1, 3, 2, 1, 1)
LAG = (3, 5)
HELD = 4
AHEAD = 4
ROOT = 1


def grouped(items, sizes):
    runs, at = [], 0
    for size in list(sizes) + [1] * len(items):
        if at < len(items):
            runs.append(items[at:at + size])
            at += size
    return runs


def turns(n):
    turn = list(range(1, n))
    turn.insert(min(4, n - 1), 0)
    return turn


def plan(n):
    turn = turns(n)
    order = []
    for j in range(n + max(LAG)):
        if j <= n:
            order.append(("a", j))
        order += [(core, turn[j - LAG[core]]) for core in (0, 1) if 0 <= j - LAG[core] < n]
    return order


def kernel(ntok, widths, x_hbm, w_hbm, ids_hbm, bias_hbm,
           wide, thin,
           xv, wv, ids, bias_all, part, rx1, keep, mine, tx2, rx2, tx3, rx3, cnt, fin,
           l_sem, s1, r1, s2, r2, s3, r3, sc, rc, rb, ready):
    half = widths[0] // 2
    units = [(sum(widths[:i]), widths[i], i) for i in range(1, len(widths))]
    for k, place in enumerate(RAW_AT):
        units.insert(place, (k * half, half, 0))
    sizes = sorted({width for _, width, _ in units})
    acc_of = [2 * sizes.index(width) + sum(w == width for _, w, _ in units[:j]) % 2
              for j, (_, width, _) in enumerate(units)]
    specs = [tuple(pltpu.ACC(q)((width, 256), F32) for q in (0, 1)) for width in sizes for _ in range(2)]
    pl.run_scoped(functools.partial(body, ntok, widths, units, acc_of, (
        x_hbm, w_hbm, ids_hbm, bias_hbm, wide, thin,
        xv, wv, ids, bias_all, part, rx1, keep, mine, tx2, rx2, tx3, rx3, cnt, fin,
        l_sem, s1, r1, s2, r2, s3, r3, sc, rc, rb, ready)), *specs)


def body(ntok, widths, units, acc_of, refs, *accs):
    (x_hbm, w_hbm, ids_hbm, bias_hbm, wide, thin,
     xv, wv, ids, bias_all, part, rx1, keep, mine, tx2, rx2, tx3, rx3, cnt, fin,
     l_sem, s1, r1, s2, r2, s3, r3, sc, rc, rb, ready) = refs
    own = bias_all.shape[2]
    top, rows = ids.shape
    depth = xv.shape[1]
    n = len(widths)
    starts = [sum(widths[:i]) for i in range(n)]
    t, e = lax.axis_index("tok"), lax.axis_index("exp")
    y, c = e // 2, e % 2
    mate = 2 * y + 1 - c
    peer = 2 * (1 - y) + c
    cross = 2 * (1 - y) + 1 - c
    experts = 4 * own
    is_root = e == ROOT
    others = [k for k in range(4) if k != ROOT]

    def cols(i):
        return pl.ds(starts[i], widths[i])

    nu = len(units)
    mate_runs, peer_runs = grouped(turns(n), MATE_RUNS), grouped(list(range(n)), PEER_RUNS)
    mate_run = {i: k for k, run in enumerate(mate_runs) for i in run}
    peer_run = {i: k for k, run in enumerate(peer_runs) for i in run}

    def unit(j):
        return pl.ds(*units[j][:2])

    def within(j):
        start, width, i = units[j]
        return pl.ds(start - starts[i], width)

    chunk = -(-depth // W_CHUNKS // 256) * 256
    chunks = [pl.ds(k, min(chunk, depth - k)) for k in range(0, depth, chunk)]
    w_in = [pltpu.make_async_copy(w_hbm.at[k], wv.at[k], l_sem.at[0]) for k in chunks]
    w_all = pltpu.make_async_copy(w_hbm, wv, l_sem.at[0])
    ids_in = pltpu.make_async_copy(ids_hbm, ids, l_sem.at[1])
    slot = [2 + i if i < AHEAD else 0 if i == AHEAD else 2 + (i - AHEAD - 1) % AHEAD for i in range(nu)]
    x_in = [pltpu.make_async_copy(x_hbm.at[unit(j)], xv.at[unit(j)], l_sem.at[slot[j]]) for j in range(nu)]
    ids_in.start()
    for copy in w_in + x_in[:AHEAD]:
        copy.start()

    barrier = pltpu.get_barrier_semaphore()

    for k in others:
        @pl.when(e != k)
        def _():
            pl.semaphore_signal(barrier, inc=1, device_id=(t, k), device_id_type=MESH)

    bias_in = pltpu.make_async_copy(bias_hbm, bias_all.at[ROOT], sc)
    bias_out = pltpu.make_async_remote_copy(
        src_ref=bias_hbm, dst_ref=bias_all.at[e], send_sem=sc, recv_sem=rb,
        device_id=(t, ROOT), device_id_type=MESH)
    bias_back = pltpu.make_async_remote_copy(
        src_ref=bias_all.at[pl.ds(0, 3)], dst_ref=bias_all.at[pl.ds(0, 3)], send_sem=sc, recv_sem=rb,
        device_id=(t, mate), device_id_type=MESH)
    cnt_out = [pltpu.make_async_remote_copy(
        src_ref=cnt.at[0], dst_ref=cnt.at[d], send_sem=sc, recv_sem=rc,
        device_id=((t + d) % ntok, e), device_id_type=MESH) for d in range(1, ntok)]
    rest = pl.ds(1, ntok - 1)
    cnt_all = pltpu.make_async_remote_copy(
        src_ref=cnt.at[rest], dst_ref=cnt.at[rest], send_sem=sc, recv_sem=rc,
        device_id=(t, mate), device_id_type=MESH)
    fin_out = [pltpu.make_async_remote_copy(
        src_ref=fin.at[j], dst_ref=fin.at[3], send_sem=sc, recv_sem=rc,
        device_id=(t, k), device_id_type=MESH) for j, k in enumerate(others)]
    fin_all = pltpu.make_async_remote_copy(
        src_ref=fin.at[pl.ds(0, 3)], dst_ref=fin.at[pl.ds(0, 3)], send_sem=sc, recv_sem=rc,
        device_id=(t, mate), device_id_type=MESH)

    @pl.when(is_root)
    def _():
        bias_in.start()
        for d in range(1, ntok):
            pl.semaphore_signal(barrier, inc=1, device_id=((t + d) % ntok, e), device_id_type=MESH)
        ids_in.wait()
        lanes = 128
        numbers = lax.broadcasted_iota(jnp.int32, (experts, lanes), 0).astype(F32).astype(jnp.bfloat16)
        one, zero = jnp.bfloat16(1), jnp.bfloat16(0)
        exact = 256 // top
        blocks = rows // lanes
        total = jnp.zeros((1, experts), F32)
        for g0 in range(0, blocks, exact):
            acc = jnp.zeros((experts, lanes), jnp.bfloat16)
            for g in range(g0, min(g0 + exact, blocks)):
                found = ids[:, pl.ds(g * lanes, lanes)].astype(F32).astype(jnp.bfloat16)
                for j in range(top):
                    acc = acc + jnp.where(found[j:j + 1] == numbers, one, zero)
            total = total + jnp.sum(acc.astype(F32).T, axis=0, keepdims=True)
        cnt[0] = total.astype(jnp.int32)
        bias_in.wait()

    @pl.when(jnp.logical_not(is_root))
    def _():
        pl.semaphore_wait(barrier, 3)
        pl.semaphore_signal(ready, inc=1, device_id=(t, ROOT), device_id_type=MESH)
        bias_out.start()
        ids_in.wait()

    queue = list(range(AHEAD, nu))

    def more_tokens(freed):
        if queue and slot[queue[0]] == freed:
            x_in[queue.pop(0)].start()

    def send_counts():
        pl.semaphore_wait(barrier, ntok - 1)
        for copy in cnt_out:
            copy.start()

    def send_counts_soon():
        pl.when(jnp.logical_and(is_root, 2 * t >= ntok))(send_counts)

    def send_counts_late():
        pl.when(jnp.logical_and(is_root, 2 * t < ntok))(send_counts)

    def finish_counts():
        @pl.when(is_root)
        def _():
            cnt_all.wait()
            bias_back.wait_recv()
            total = cnt[0]
            for d in range(1, ntok):
                total = total + cnt[d]
            load = total.astype(F32)
            target = F32(ntok * rows * top)
            gap = target - F32(experts) * load
            sign = jnp.where(gap > 0, F32(1), jnp.where(gap < 0, F32(-1), F32(0)))
            bias = jnp.concatenate([bias_all[k] for k in range(4)], axis=1)
            for j in range(4):
                fin[j, 0] = load
                fin[j, 1] = bias + 0.001 * sign
            for copy in fin_out:
                copy.start()

    def close_counts():
        @pl.when(is_root)
        def _():
            fin_all.wait_send()

        @pl.when(jnp.logical_not(is_root))
        def _():
            fin_out[0].wait_recv()
            bias_out.wait_send()

        thin[...] = fin[3]

    def first(at, k):
        return pltpu.make_async_remote_copy(
            src_ref=part.at[1 - c, at], dst_ref=rx1.at[at],
            send_sem=s1, recv_sem=r1.at[k], device_id=(t, mate), device_id_type=MESH)

    def second(at, k):
        return pltpu.make_async_remote_copy(
            src_ref=tx2.at[at], dst_ref=rx2.at[at],
            send_sem=s2, recv_sem=r2.at[k], device_id=(t, peer), device_id_type=MESH)

    def raw(j):
        return pltpu.make_async_remote_copy(
            src_ref=tx2.at[0, :, within(j)], dst_ref=rx2.at[0, :, within(j)],
            send_sem=s2, recv_sem=r2.at[0], device_id=(t, peer), device_id_type=MESH)

    def across(j):
        return pltpu.make_async_remote_copy(
            src_ref=tx2.at[n, :, within(j)], dst_ref=rx2.at[n, :, within(j)],
            send_sem=s2, recv_sem=r2.at[0], device_id=(t, cross), device_id_type=MESH)

    chosen_out = pltpu.make_async_remote_copy(
        src_ref=tx3, dst_ref=rx3, send_sem=s3, recv_sem=r3, device_id=(t, peer), device_id_type=MESH)
    hand_on = pltpu.make_async_remote_copy(
        src_ref=rx3, dst_ref=rx3, send_sem=s3, recv_sem=r3, device_id=(t, mate), device_id_type=MESH)

    def arrival(i, runs, copy, blocks):
        for k, run in enumerate(runs):
            if run[0] == i:
                copy(pl.ds(0, sum(blocks(m) for m in run)), k).wait_recv()

    side = 256
    tiles = depth // side
    shares = [[(q, k) for q in (0, 1) for k in range(tiles)
               if (k < (tiles + 1 - i % 2) // 2) == (q == 0)] for i in range(nu)]
    line = [[(i, k) for i in range(nu) for p, k in shares[i] if p == q] for q in (0, 1)]
    where = [0, 0]

    def push(q):
        if where[q] < len(line[q]):
            k = line[q][where[q]][1]
            pltpu.matmul_push_rhs(wv[pl.ds(k * side, side), :], staging_register=where[q] % 2, mxu_index=q)

    def issue(i):
        x_in[i].wait()
        more_tokens(slot[i])
        left = [[k for p, k in shares[i] if p == q] for q in (0, 1)]
        for step in range(max(map(len, left))):
            for q in (0, 1):
                if step < len(left[q]):
                    k = left[q][step]
                    mark = where[q] % 2
                    where[q] += 1
                    push(q)
                    pltpu.matmul_acc_lhs(accs[acc_of[i]][q], xv[unit(i), pl.ds(k * side, side)], load_staged_rhs=mark)

    def product(j):
        if 0 < j < nu - 1:
            issue(j + 1)
        r = (pltpu.matmul_pop(accs[acc_of[j]][0]) + pltpu.matmul_pop(accs[acc_of[j]][1])).T
        for k in range(4):
            part[k % 2, units[j][2], pl.ds(k // 2 * own, own), within(j)] = r[k * own:(k + 1) * own]

    def pick(i):
        mine_ids = ids[:, cols(i)]
        low, high = mine_ids & 7, mine_ids >> 3
        picked = jnp.zeros(mine_ids.shape, F32)
        for k in range(experts // 8):
            block, line = divmod(8 * k, own)
            rows8 = part[block % 2, i, pl.ds(block // 2 * own + line, 8), :]
            row = jnp.take_along_axis(rows8, low, axis=0, mode="promise_in_bounds")
            picked = jnp.where(high == k, row, picked)
        for k in range(2):
            part[k, i, pl.ds(2 * own, top), :] = picked

    def to_mate(i):
        pick(i)
        first(i, mate_run[i]).start()

    def stage_a(j):
        product(j)
        if j == 0:
            @pl.when(is_root)
            def _():
                pl.semaphore_wait(ready, 3)
        start, width, i = units[j]
        if i == 0:
            tx2[0, :, within(j)] = encode(part[c, 0, theirs, within(j)]).astype(LINK)
            tx2[n, :, within(j)] = encode(part[1 - c, 0, theirs, within(j)]).astype(LINK)
            raw(j).start()
            across(j).start()
        else:
            to_mate(i)
        if j == 0:
            issue(1)
        if j == RAW_AT[-1] + 1:
            to_mate(0)

    bound = 2 * depth * TOKEN_BOUND * GATE_BOUND
    grain = TOP_CODE / math.asinh(bound)

    def encode(v):
        size = jnp.abs(v)
        code = jnp.log(size + jnp.sqrt(size * size + F32(1))) * F32(grain) + F32(0.5)
        return jnp.where(v < 0, -code, code).astype(jnp.int32)

    def decode(whole):
        grown = jnp.exp(whole.astype(F32) * F32(1 / grain))
        return F32(0.5) * grown - F32(0.5) / grown

    theirs = pl.ds(pl.multiple_of((1 - y) * own, own), own)
    ours = pl.ds(pl.multiple_of(y * own, own), own)
    picks = pl.ds(2 * own, top)

    def stage_b(i, core):
        arrival(i, mate_runs, first, lambda m: 1)
        if i > 0:
            tx2[i] = encode(part[c, i, theirs] + rx1[i, theirs]).astype(LINK)
            if core == 0 or i < n - HELD:
                second(i, peer_run[i]).start()
        chosen = encode(part[c, i, picks] + rx1[i, picks])
        if core == 1:
            tx3[:, cols(i)] = chosen.astype(LINK)
        if core == 1 and i == n - 1:
            chosen_out.start()
            for k in range(n - HELD, n):
                second(k, peer_run[k]).start()
        keep[:, cols(i)] = part[c, i, ours] + rx1[i, ours]
        mine[:, cols(i)] = decode(chosen)

    def weigh():
        chosen = 1.0 / (1.0 + jnp.exp(-(mine[...] + decode(rx3[...].astype(jnp.int32)))))
        wide[own:] = 2.5 * chosen / jnp.sum(chosen, axis=0, keepdims=True)

    def stage_c(i):
        arrival(i, peer_runs, second, lambda m: 2 if m == 0 else 1)
        logits = keep[:, cols(i)] + decode(rx2[i].astype(jnp.int32))
        if i == 0:
            logits = logits + decode(rx2[n].astype(jnp.int32))
        wide[0:own, cols(i)] = 1.0 / (1.0 + jnp.exp(-logits))

    w_all.wait()
    more_tokens(0)
    for q in (0, 1):
        push(q)
    issue(0)
    for kind, i in plan(n):
        if kind == "a":
            stage_a(i)
        else:
            pl.when(c == kind)(functools.partial(stage_b, i, kind))
        if (kind, i) == ("a", 1):
            send_counts_soon()
        if (kind, i) == ("a", n):
            send_counts_late()
    for i in range(n):
        if i == n - HELD:
            @pl.when(c == 1)
            def _():
                chosen_out.wait()
                hand_on.start()
            finish_counts()
        if i == n - 1:
            pl.when(c == 0)(hand_on.wait_recv)
            weigh()
        stage_c(i)
    close_counts()
    first(pl.ds(0, n), 0).wait_send()
    second(pl.ds(0, n + 1), 0).wait_send()
    pl.when(c == 1)(hand_on.wait_send)


def place(wide, thin, aff_hbm, wts_hbm, load_hbm, newb_hbm, sem):
    for k, (source, results) in enumerate(((wide, (aff_hbm, wts_hbm)), (thin, (load_hbm, newb_hbm)))):
        at = 0
        for result in results:
            pltpu.make_async_copy(source.at[pl.ds(at, result.shape[0])], result, sem.at[k]).start()
            at += result.shape[0]
    for k, source in enumerate((wide, thin)):
        pltpu.make_async_copy(source, source, sem.at[k]).wait()


def local(ntok, tokens, gate_weight, expert_ids, expert_bias):
    rows, depth = tokens.shape
    experts = gate_weight.shape[1]
    own = expert_bias.shape[0]
    top = expert_ids.shape[1]
    piece = 256
    widths = [piece] * (rows // piece)
    n = len(widths)
    dma = pltpu.SemaphoreType.DMA
    vm = pltpu.VMEM
    any_ = pl.BlockSpec(memory_space=pl.ANY)
    vmem = pl.BlockSpec(memory_space=pltpu.VMEM)
    shapes = ((own, rows), (top, rows), (1, 1, experts), (1, 1, experts))
    results = pl.pallas_call(
        functools.partial(kernel, ntok, widths),
        out_shape=(pltpu.VMEM((own + top, rows), F32), pltpu.VMEM((2, 1, experts), F32)),
        in_specs=[any_] * 4,
        out_specs=(vmem,) * 2,
        scratch_shapes=[
            vm((rows, depth), tokens.dtype), vm((depth, experts), gate_weight.dtype),
            vm((top, rows), jnp.int32),
            vm((4, 1, own), F32),
            vm((2, n, 2 * own + top, piece), F32), vm((n, 2 * own + top, piece), F32),
            vm((own, rows), F32), vm((top, rows), F32),
            vm((n + 1, own, piece), LINK), vm((n + 1, own, piece), LINK),
            vm((top, rows), LINK), vm((top, rows), LINK),
            vm((ntok, 1, experts), jnp.int32), vm((4, 2, 1, experts), F32),
            dma((2 + AHEAD,)), dma, dma((len(grouped(turns(n), MATE_RUNS)),)),
            dma, dma((len(grouped(turns(n), PEER_RUNS)),)), dma, dma, dma, dma, dma,
            pltpu.SemaphoreType.REGULAR,
        ],
        compiler_params=pltpu.CompilerParams(
            collective_id=0, has_side_effects=True, vmem_limit_bytes=60 * 1024 * 1024),
    )(tokens, gate_weight, expert_ids.T, expert_bias.reshape(1, own))
    aff, wts, load, newb = pl.pallas_call(
        place,
        out_shape=tuple(jax.ShapeDtypeStruct(shape, F32) for shape in shapes),
        in_specs=[vmem] * 2,
        out_specs=(pl.BlockSpec(memory_space=pltpu.HBM),) * 4,
        scratch_shapes=[dma((2,))],
    )(*(pltpu.with_memory_space_constraint(r, pltpu.VMEM) for r in results))
    return aff.T, wts.T, load.reshape(experts), newb.reshape(experts)


def solution(mesh):
    in_specs = (P("tok", "exp"), P("exp", None), P("tok", None), P("exp"))
    out_specs = (P("tok", "exp"), P("tok", None), P(), P())
    return jax.shard_map(functools.partial(local, mesh.shape["tok"]), mesh=mesh,
                         in_specs=in_specs, out_specs=out_specs, check_vma=False)
```

```python
import functools
import math

import jax
import jax.numpy as jnp
from jax import lax
from jax.experimental import pallas as pl
from jax.experimental.pallas import tpu as pltpu
from jax.sharding import PartitionSpec as P

MESH = pl.DeviceIdType.MESH
F32 = jnp.float32
LINK = jnp.int16
TOP_CODE = 32760.0
TOKEN_BOUND, GATE_BOUND = 6.0, 0.0625
W_CHUNKS = 4
RAW_AT = (0, 2)
MATE_RUNS = (1, 1, 1, 2, 1, 2)
PEER_RUNS = (1, 3, 2, 1, 1)
LAG = (3, 5)
HELD = 4
AHEAD = 4
ROOT = 1


def grouped(items, sizes):
    runs, at = [], 0
    for size in list(sizes) + [1] * len(items):
        if at < len(items):
            runs.append(items[at:at + size])
            at += size
    return runs


def turns(n):
    turn = list(range(1, n))
    turn.insert(min(4, n - 1), 0)
    return turn


def plan(n):
    turn = turns(n)
    order = []
    for j in range(n + max(LAG)):
        if j <= n:
            order.append(("a", j))
        order += [(core, turn[j - LAG[core]]) for core in (0, 1) if 0 <= j - LAG[core] < n]
    return order


def kernel(ntok, widths, x_hbm, w_hbm, ids_hbm, bias_hbm,
           wide, thin,
           xv, wv, ids, bias_all, part, rx1, keep, mine, tx2, rx2, tx3, rx3, cnt, fin,
           l_sem, s1, r1, s2, r2, s3, r3, sc, rc, rb, ready):
    half = widths[0] // 2
    units = [(sum(widths[:i]), widths[i], i) for i in range(1, len(widths))]
    for k, place in enumerate(RAW_AT):
        units.insert(place, (k * half, half, 0))
    sizes = sorted({width for _, width, _ in units})
    acc_of = [2 * sizes.index(width) + sum(w == width for _, w, _ in units[:j]) % 2
              for j, (_, width, _) in enumerate(units)]
    specs = [tuple(pltpu.ACC(q)((width, 256), F32) for q in (0, 1)) for width in sizes for _ in range(2)]
    pl.run_scoped(functools.partial(body, ntok, widths, units, acc_of, (
        x_hbm, w_hbm, ids_hbm, bias_hbm, wide, thin,
        xv, wv, ids, bias_all, part, rx1, keep, mine, tx2, rx2, tx3, rx3, cnt, fin,
        l_sem, s1, r1, s2, r2, s3, r3, sc, rc, rb, ready)), *specs)


def body(ntok, widths, units, acc_of, refs, *accs):
    (x_hbm, w_hbm, ids_hbm, bias_hbm, wide, thin,
     xv, wv, ids, bias_all, part, rx1, keep, mine, tx2, rx2, tx3, rx3, cnt, fin,
     l_sem, s1, r1, s2, r2, s3, r3, sc, rc, rb, ready) = refs
    own = bias_all.shape[2]
    top, rows = ids.shape
    depth = xv.shape[1]
    n = len(widths)
    starts = [sum(widths[:i]) for i in range(n)]
    t, e = lax.axis_index("tok"), lax.axis_index("exp")
    y, c = e // 2, e % 2
    mate = 2 * y + 1 - c
    peer = 2 * (1 - y) + c
    cross = 2 * (1 - y) + 1 - c
    experts = 4 * own
    is_root = e == ROOT
    others = [k for k in range(4) if k != ROOT]

    def cols(i):
        return pl.ds(starts[i], widths[i])

    nu = len(units)
    mate_runs, peer_runs = grouped(turns(n), MATE_RUNS), grouped(list(range(n)), PEER_RUNS)
    mate_run = {i: k for k, run in enumerate(mate_runs) for i in run}
    peer_run = {i: k for k, run in enumerate(peer_runs) for i in run}

    def unit(j):
        return pl.ds(*units[j][:2])

    def within(j):
        start, width, i = units[j]
        return pl.ds(start - starts[i], width)

    chunk = -(-depth // W_CHUNKS // 256) * 256
    chunks = [pl.ds(k, min(chunk, depth - k)) for k in range(0, depth, chunk)]
    w_in = [pltpu.make_async_copy(w_hbm.at[k], wv.at[k], l_sem.at[0]) for k in chunks]
    w_all = pltpu.make_async_copy(w_hbm, wv, l_sem.at[0])
    ids_in = pltpu.make_async_copy(ids_hbm, ids, l_sem.at[1])
    slot = [2 + i if i < AHEAD else 0 if i == AHEAD else 2 + (i - AHEAD - 1) % AHEAD for i in range(nu)]
    x_in = [pltpu.make_async_copy(x_hbm.at[unit(j)], xv.at[unit(j)], l_sem.at[slot[j]]) for j in range(nu)]
    ids_in.start()
    for copy in w_in + x_in[:AHEAD]:
        copy.start()

    barrier = pltpu.get_barrier_semaphore()

    for k in others:
        @pl.when(e != k)
        def _():
            pl.semaphore_signal(barrier, inc=1, device_id=(t, k), device_id_type=MESH)

    bias_in = pltpu.make_async_copy(bias_hbm, bias_all.at[ROOT], sc)
    bias_out = pltpu.make_async_remote_copy(
        src_ref=bias_hbm, dst_ref=bias_all.at[e], send_sem=sc, recv_sem=rb,
        device_id=(t, ROOT), device_id_type=MESH)
    bias_back = pltpu.make_async_remote_copy(
        src_ref=bias_all.at[pl.ds(0, 3)], dst_ref=bias_all.at[pl.ds(0, 3)], send_sem=sc, recv_sem=rb,
        device_id=(t, mate), device_id_type=MESH)
    cnt_out = [pltpu.make_async_remote_copy(
        src_ref=cnt.at[0], dst_ref=cnt.at[d], send_sem=sc, recv_sem=rc,
        device_id=((t + d) % ntok, e), device_id_type=MESH) for d in range(1, ntok)]
    rest = pl.ds(1, ntok - 1)
    cnt_all = pltpu.make_async_remote_copy(
        src_ref=cnt.at[rest], dst_ref=cnt.at[rest], send_sem=sc, recv_sem=rc,
        device_id=(t, mate), device_id_type=MESH)
    fin_out = [pltpu.make_async_remote_copy(
        src_ref=fin.at[j], dst_ref=fin.at[3], send_sem=sc, recv_sem=rc,
        device_id=(t, k), device_id_type=MESH) for j, k in enumerate(others)]
    fin_all = pltpu.make_async_remote_copy(
        src_ref=fin.at[pl.ds(0, 3)], dst_ref=fin.at[pl.ds(0, 3)], send_sem=sc, recv_sem=rc,
        device_id=(t, mate), device_id_type=MESH)

    @pl.when(is_root)
    def _():
        bias_in.start()
        for d in range(1, ntok):
            pl.semaphore_signal(barrier, inc=1, device_id=((t + d) % ntok, e), device_id_type=MESH)
        ids_in.wait()
        lanes = 128
        numbers = lax.broadcasted_iota(jnp.int32, (experts, lanes), 0).astype(F32).astype(jnp.bfloat16)
        one, zero = jnp.bfloat16(1), jnp.bfloat16(0)
        exact = 256 // top
        blocks = rows // lanes
        total = jnp.zeros((1, experts), F32)
        for g0 in range(0, blocks, exact):
            acc = jnp.zeros((experts, lanes), jnp.bfloat16)
            for g in range(g0, min(g0 + exact, blocks)):
                found = ids[:, pl.ds(g * lanes, lanes)].astype(F32).astype(jnp.bfloat16)
                for j in range(top):
                    acc = acc + jnp.where(found[j:j + 1] == numbers, one, zero)
            total = total + jnp.sum(acc.astype(F32).T, axis=0, keepdims=True)
        cnt[0] = total.astype(jnp.int32)
        bias_in.wait()

    @pl.when(jnp.logical_not(is_root))
    def _():
        pl.semaphore_wait(barrier, 3)
        pl.semaphore_signal(ready, inc=1, device_id=(t, ROOT), device_id_type=MESH)
        bias_out.start()
        ids_in.wait()

    queue = list(range(AHEAD, nu))

    def more_tokens(freed):
        if queue and slot[queue[0]] == freed:
            x_in[queue.pop(0)].start()

    def send_counts():
        pl.semaphore_wait(barrier, ntok - 1)
        for copy in cnt_out:
            copy.start()

    def send_counts_soon():
        pl.when(jnp.logical_and(is_root, 2 * t >= ntok))(send_counts)

    def send_counts_late():
        pl.when(jnp.logical_and(is_root, 2 * t < ntok))(send_counts)

    def finish_counts():
        @pl.when(is_root)
        def _():
            cnt_all.wait()
            bias_back.wait_recv()
            total = cnt[0]
            for d in range(1, ntok):
                total = total + cnt[d]
            load = total.astype(F32)
            target = F32(ntok * rows * top)
            gap = target - F32(experts) * load
            sign = jnp.where(gap > 0, F32(1), jnp.where(gap < 0, F32(-1), F32(0)))
            bias = jnp.concatenate([bias_all[k] for k in range(4)], axis=1)
            for j in range(4):
                fin[j, 0] = load
                fin[j, 1] = bias + 0.001 * sign
            for copy in fin_out:
                copy.start()

    def close_counts():
        @pl.when(is_root)
        def _():
            fin_all.wait_send()

        @pl.when(jnp.logical_not(is_root))
        def _():
            fin_out[0].wait_recv()
            bias_out.wait_send()

        thin[...] = fin[3]

    def first(at, k):
        return pltpu.make_async_remote_copy(
            src_ref=part.at[1 - c, at], dst_ref=rx1.at[at],
            send_sem=s1, recv_sem=r1.at[k], device_id=(t, mate), device_id_type=MESH)

    def second(at, k):
        return pltpu.make_async_remote_copy(
            src_ref=tx2.at[at], dst_ref=rx2.at[at],
            send_sem=s2, recv_sem=r2.at[k], device_id=(t, peer), device_id_type=MESH)

    def raw(j):
        return pltpu.make_async_remote_copy(
            src_ref=tx2.at[0, :, within(j)], dst_ref=rx2.at[0, :, within(j)],
            send_sem=s2, recv_sem=r2.at[0], device_id=(t, peer), device_id_type=MESH)

    def across(j):
        return pltpu.make_async_remote_copy(
            src_ref=tx2.at[n, :, within(j)], dst_ref=rx2.at[n, :, within(j)],
            send_sem=s2, recv_sem=r2.at[0], device_id=(t, cross), device_id_type=MESH)

    chosen_out = pltpu.make_async_remote_copy(
        src_ref=tx3, dst_ref=rx3, send_sem=s3, recv_sem=r3, device_id=(t, peer), device_id_type=MESH)
    hand_on = pltpu.make_async_remote_copy(
        src_ref=rx3, dst_ref=rx3, send_sem=s3, recv_sem=r3, device_id=(t, mate), device_id_type=MESH)

    def arrival(i, runs, copy, blocks):
        for k, run in enumerate(runs):
            if run[0] == i:
                copy(pl.ds(0, sum(blocks(m) for m in run)), k).wait_recv()

    side = 256
    tiles = depth // side
    shares = [[(q, k) for q in (0, 1) for k in range(tiles)
               if (k < (tiles + 1 - i % 2) // 2) == (q == 0)] for i in range(nu)]
    line = [[(i, k) for i in range(nu) for p, k in shares[i] if p == q] for q in (0, 1)]
    where = [0, 0]

    def push(q):
        if where[q] < len(line[q]):
            k = line[q][where[q]][1]
            pltpu.matmul_push_rhs(wv[pl.ds(k * side, side), :], staging_register=where[q] % 2, mxu_index=q)

    def issue(i):
        x_in[i].wait()
        more_tokens(slot[i])
        left = [[k for p, k in shares[i] if p == q] for q in (0, 1)]
        for step in range(max(map(len, left))):
            for q in (0, 1):
                if step < len(left[q]):
                    k = left[q][step]
                    mark = where[q] % 2
                    where[q] += 1
                    push(q)
                    pltpu.matmul_acc_lhs(accs[acc_of[i]][q], xv[unit(i), pl.ds(k * side, side)], load_staged_rhs=mark)

    def product(j):
        if 0 < j < nu - 1:
            issue(j + 1)
        r = (pltpu.matmul_pop(accs[acc_of[j]][0]) + pltpu.matmul_pop(accs[acc_of[j]][1])).T
        for k in range(4):
            part[k % 2, units[j][2], pl.ds(k // 2 * own, own), within(j)] = r[k * own:(k + 1) * own]

    def pick(i):
        mine_ids = ids[:, cols(i)]
        low, high = mine_ids & 7, mine_ids >> 3
        picked = jnp.zeros(mine_ids.shape, F32)
        for k in range(experts // 8):
            block, line = divmod(8 * k, own)
            rows8 = part[block % 2, i, pl.ds(block // 2 * own + line, 8), :]
            row = jnp.take_along_axis(rows8, low, axis=0, mode="promise_in_bounds")
            picked = jnp.where(high == k, row, picked)
        for k in range(2):
            part[k, i, pl.ds(2 * own, top), :] = picked

    def to_mate(i):
        pick(i)
        first(i, mate_run[i]).start()

    def stage_a(j):
        product(j)
        if j == 0:
            @pl.when(is_root)
            def _():
                pl.semaphore_wait(ready, 3)
        start, width, i = units[j]
        if i == 0:
            tx2[0, :, within(j)] = encode(part[c, 0, theirs, within(j)]).astype(LINK)
            tx2[n, :, within(j)] = encode(part[1 - c, 0, theirs, within(j)]).astype(LINK)
            raw(j).start()
            across(j).start()
        else:
            to_mate(i)
        if j == 0:
            issue(1)
        if j == RAW_AT[-1] + 1:
            to_mate(0)

    bound = 2 * depth * TOKEN_BOUND * GATE_BOUND
    grain = TOP_CODE / math.asinh(bound)

    def encode(v):
        size = jnp.abs(v)
        code = jnp.log(size + jnp.sqrt(size * size + F32(1))) * F32(grain) + F32(0.5)
        return jnp.where(v < 0, -code, code).astype(jnp.int32)

    def decode(whole):
        grown = jnp.exp(whole.astype(F32) * F32(1 / grain))
        return F32(0.5) * grown - F32(0.5) / grown

    theirs = pl.ds(pl.multiple_of((1 - y) * own, own), own)
    ours = pl.ds(pl.multiple_of(y * own, own), own)
    picks = pl.ds(2 * own, top)

    def stage_b(i, core):
        arrival(i, mate_runs, first, lambda m: 1)
        if i > 0:
            tx2[i] = encode(part[c, i, theirs] + rx1[i, theirs]).astype(LINK)
            if core == 0 or i < n - HELD:
                second(i, peer_run[i]).start()
        chosen = encode(part[c, i, picks] + rx1[i, picks])
        if core == 1:
            tx3[:, cols(i)] = chosen.astype(LINK)
        if core == 1 and i == n - 1:
            chosen_out.start()
            for k in range(n - HELD, n):
                second(k, peer_run[k]).start()
        keep[:, cols(i)] = part[c, i, ours] + rx1[i, ours]
        mine[:, cols(i)] = decode(chosen)

    def weigh():
        chosen = 1.0 / (1.0 + jnp.exp(-(mine[...] + decode(rx3[...].astype(jnp.int32)))))
        wide[own:] = 2.5 * chosen / jnp.sum(chosen, axis=0, keepdims=True)

    def stage_c(i):
        arrival(i, peer_runs, second, lambda m: 2 if m == 0 else 1)
        logits = keep[:, cols(i)] + decode(rx2[i].astype(jnp.int32))
        if i == 0:
            logits = logits + decode(rx2[n].astype(jnp.int32))
        wide[0:own, cols(i)] = 1.0 / (1.0 + jnp.exp(-logits))

    w_all.wait()
    more_tokens(0)
    for q in (0, 1):
        push(q)
    issue(0)
    for kind, i in plan(n):
        if kind == "a":
            stage_a(i)
        else:
            pl.when(c == kind)(functools.partial(stage_b, i, kind))
        if (kind, i) == ("a", 1):
            send_counts_soon()
        if (kind, i) == ("a", n):
            send_counts_late()
    for i in range(n):
        if i == n - HELD:
            @pl.when(c == 1)
            def _():
                chosen_out.wait()
                hand_on.start()
            finish_counts()
        if i == n - 1:
            pl.when(c == 0)(hand_on.wait_recv)
            weigh()
            close_counts()
            first(pl.ds(0, n), 0).wait_send()
            second(pl.ds(0, n + 1), 0).wait_send()
            pl.when(c == 1)(hand_on.wait_send)
        stage_c(i)


def place(wide, thin, aff_hbm, wts_hbm, load_hbm, newb_hbm, sem):
    for k, (source, results) in enumerate(((wide, (aff_hbm, wts_hbm)), (thin, (load_hbm, newb_hbm)))):
        at = 0
        for result in results:
            pltpu.make_async_copy(source.at[pl.ds(at, result.shape[0])], result, sem.at[k]).start()
            at += result.shape[0]
    for k, source in enumerate((wide, thin)):
        pltpu.make_async_copy(source, source, sem.at[k]).wait()


def local(ntok, tokens, gate_weight, expert_ids, expert_bias):
    rows, depth = tokens.shape
    experts = gate_weight.shape[1]
    own = expert_bias.shape[0]
    top = expert_ids.shape[1]
    piece = 256
    widths = [piece] * (rows // piece)
    n = len(widths)
    dma = pltpu.SemaphoreType.DMA
    vm = pltpu.VMEM
    any_ = pl.BlockSpec(memory_space=pl.ANY)
    vmem = pl.BlockSpec(memory_space=pltpu.VMEM)
    shapes = ((own, rows), (top, rows), (1, 1, experts), (1, 1, experts))
    results = pl.pallas_call(
        functools.partial(kernel, ntok, widths),
        out_shape=(pltpu.VMEM((own + top, rows), F32), pltpu.VMEM((2, 1, experts), F32)),
        in_specs=[any_] * 4,
        out_specs=(vmem,) * 2,
        scratch_shapes=[
            vm((rows, depth), tokens.dtype), vm((depth, experts), gate_weight.dtype),
            vm((top, rows), jnp.int32),
            vm((4, 1, own), F32),
            vm((2, n, 2 * own + top, piece), F32), vm((n, 2 * own + top, piece), F32),
            vm((own, rows), F32), vm((top, rows), F32),
            vm((n + 1, own, piece), LINK), vm((n + 1, own, piece), LINK),
            vm((top, rows), LINK), vm((top, rows), LINK),
            vm((ntok, 1, experts), jnp.int32), vm((4, 2, 1, experts), F32),
            dma((2 + AHEAD,)), dma, dma((len(grouped(turns(n), MATE_RUNS)),)),
            dma, dma((len(grouped(turns(n), PEER_RUNS)),)), dma, dma, dma, dma, dma,
            pltpu.SemaphoreType.REGULAR,
        ],
        compiler_params=pltpu.CompilerParams(
            collective_id=0, has_side_effects=True, vmem_limit_bytes=60 * 1024 * 1024),
    )(tokens, gate_weight, expert_ids.T, expert_bias.reshape(1, own))
    aff, wts, load, newb = pl.pallas_call(
        place,
        out_shape=tuple(jax.ShapeDtypeStruct(shape, F32) for shape in shapes),
        in_specs=[vmem] * 2,
        out_specs=(pl.BlockSpec(memory_space=pltpu.HBM),) * 4,
        scratch_shapes=[dma((2,))],
    )(*(pltpu.with_memory_space_constraint(r, pltpu.VMEM) for r in results))
    return aff.T, wts.T, load.reshape(experts), newb.reshape(experts)


def solution(mesh):
    in_specs = (P("tok", "exp"), P("exp", None), P("tok", None), P("exp"))
    out_specs = (P("tok", "exp"), P("tok", None), P(), P())
    return jax.shard_map(functools.partial(local, mesh.shape["tok"]), mesh=mesh,
                         in_specs=in_specs, out_specs=out_specs, check_vma=False)
```

```python
import functools
import math

import jax
import jax.numpy as jnp
from jax import lax
from jax.experimental import pallas as pl
from jax.experimental.pallas import tpu as pltpu
from jax.sharding import PartitionSpec as P

MESH = pl.DeviceIdType.MESH
F32 = jnp.float32
LINK = jnp.int16
TOP_CODE = 32760.0
TOKEN_BOUND, GATE_BOUND = 6.0, 0.0625
W_CHUNKS = 2
RAW_AT = (0, 2)
MATE_RUNS = (1, 1, 1, 2, 1, 2)
PEER_RUNS = (1, 3, 2, 1, 1)
LAG = (3, 5)
HELD = 4
AHEAD = 5
ROOT = 1


def grouped(items, sizes):
    runs, at = [], 0
    for size in list(sizes) + [1] * len(items):
        if at < len(items):
            runs.append(items[at:at + size])
            at += size
    return runs


def turns(n):
    turn = list(range(1, n))
    turn.insert(min(4, n - 1), 0)
    return turn


def plan(n):
    turn = turns(n)
    order = []
    for j in range(n + max(LAG)):
        if j <= n:
            order.append(("a", j))
        order += [(core, turn[j - LAG[core]]) for core in (0, 1) if 0 <= j - LAG[core] < n]
    return order


def kernel(ntok, widths, x_hbm, w_hbm, ids_hbm, bias_hbm,
           wide, thin,
           xv, wv, ids, bias_all, part, rx1, keep, mine, tx2, rx2, tx3, rx3, cnt, fin,
           l_sem, s1, r1, s2, r2, s3, r3, sc, rc, rb, ready):
    half = widths[0] // 2
    units = [(sum(widths[:i]), widths[i], i) for i in range(1, len(widths))]
    for k, place in enumerate(RAW_AT):
        units.insert(place, (k * half, half, 0))
    sizes = sorted({width for _, width, _ in units})
    acc_of = [2 * sizes.index(width) + sum(w == width for _, w, _ in units[:j]) % 2
              for j, (_, width, _) in enumerate(units)]
    specs = [tuple(pltpu.ACC(q)((width, 256), F32) for q in (0, 1)) for width in sizes for _ in range(2)]
    pl.run_scoped(functools.partial(body, ntok, widths, units, acc_of, (
        x_hbm, w_hbm, ids_hbm, bias_hbm, wide, thin,
        xv, wv, ids, bias_all, part, rx1, keep, mine, tx2, rx2, tx3, rx3, cnt, fin,
        l_sem, s1, r1, s2, r2, s3, r3, sc, rc, rb, ready)), *specs)


def body(ntok, widths, units, acc_of, refs, *accs):
    (x_hbm, w_hbm, ids_hbm, bias_hbm, wide, thin,
     xv, wv, ids, bias_all, part, rx1, keep, mine, tx2, rx2, tx3, rx3, cnt, fin,
     l_sem, s1, r1, s2, r2, s3, r3, sc, rc, rb, ready) = refs
    own = bias_all.shape[2]
    top, rows = ids.shape
    depth = xv.shape[1]
    n = len(widths)
    starts = [sum(widths[:i]) for i in range(n)]
    t, e = lax.axis_index("tok"), lax.axis_index("exp")
    y, c = e // 2, e % 2
    mate = 2 * y + 1 - c
    peer = 2 * (1 - y) + c
    cross = 2 * (1 - y) + 1 - c
    experts = 4 * own
    is_root = e == ROOT
    others = [k for k in range(4) if k != ROOT]

    def cols(i):
        return pl.ds(starts[i], widths[i])

    nu = len(units)
    mate_runs, peer_runs = grouped(turns(n), MATE_RUNS), grouped(list(range(n)), PEER_RUNS)
    mate_run = {i: k for k, run in enumerate(mate_runs) for i in run}
    peer_run = {i: k for k, run in enumerate(peer_runs) for i in run}

    def unit(j):
        return pl.ds(*units[j][:2])

    def within(j):
        start, width, i = units[j]
        return pl.ds(start - starts[i], width)

    chunk = -(-depth // W_CHUNKS // 256) * 256
    chunks = [pl.ds(k, min(chunk, depth - k)) for k in range(0, depth, chunk)]
    w_in = [pltpu.make_async_copy(w_hbm.at[k], wv.at[k], l_sem.at[0]) for k in chunks]
    w_all = pltpu.make_async_copy(w_hbm, wv, l_sem.at[0])
    ids_in = pltpu.make_async_copy(ids_hbm, ids, l_sem.at[1])
    slot = [2 + i if i < AHEAD else 0 if i == AHEAD else 2 + (i - AHEAD - 1) % AHEAD for i in range(nu)]
    x_in = [pltpu.make_async_copy(x_hbm.at[unit(j)], xv.at[unit(j)], l_sem.at[slot[j]]) for j in range(nu)]
    ids_in.start()
    for copy in w_in + x_in[:AHEAD]:
        copy.start()

    barrier = pltpu.get_barrier_semaphore()

    for k in others:
        @pl.when(e != k)
        def _():
            pl.semaphore_signal(barrier, inc=1, device_id=(t, k), device_id_type=MESH)

    bias_in = pltpu.make_async_copy(bias_hbm, bias_all.at[ROOT], sc)
    bias_out = pltpu.make_async_remote_copy(
        src_ref=bias_hbm, dst_ref=bias_all.at[e], send_sem=sc, recv_sem=rb,
        device_id=(t, ROOT), device_id_type=MESH)
    bias_back = pltpu.make_async_remote_copy(
        src_ref=bias_all.at[pl.ds(0, 3)], dst_ref=bias_all.at[pl.ds(0, 3)], send_sem=sc, recv_sem=rb,
        device_id=(t, mate), device_id_type=MESH)
    cnt_out = [pltpu.make_async_remote_copy(
        src_ref=cnt.at[0], dst_ref=cnt.at[d], send_sem=sc, recv_sem=rc,
        device_id=((t + d) % ntok, e), device_id_type=MESH) for d in range(1, ntok)]
    rest = pl.ds(1, ntok - 1)
    cnt_all = pltpu.make_async_remote_copy(
        src_ref=cnt.at[rest], dst_ref=cnt.at[rest], send_sem=sc, recv_sem=rc,
        device_id=(t, mate), device_id_type=MESH)
    fin_out = [pltpu.make_async_remote_copy(
        src_ref=fin.at[j], dst_ref=fin.at[3], send_sem=sc, recv_sem=rc,
        device_id=(t, k), device_id_type=MESH) for j, k in enumerate(others)]
    fin_all = pltpu.make_async_remote_copy(
        src_ref=fin.at[pl.ds(0, 3)], dst_ref=fin.at[pl.ds(0, 3)], send_sem=sc, recv_sem=rc,
        device_id=(t, mate), device_id_type=MESH)

    @pl.when(is_root)
    def _():
        bias_in.start()
        for d in range(1, ntok):
            pl.semaphore_signal(barrier, inc=1, device_id=((t + d) % ntok, e), device_id_type=MESH)
        ids_in.wait()
        lanes = 128
        numbers = lax.broadcasted_iota(jnp.int32, (experts, lanes), 0).astype(F32).astype(jnp.bfloat16)
        one, zero = jnp.bfloat16(1), jnp.bfloat16(0)
        exact = 256 // top
        blocks = rows // lanes
        total = jnp.zeros((1, experts), F32)
        for g0 in range(0, blocks, exact):
            acc = jnp.zeros((experts, lanes), jnp.bfloat16)
            for g in range(g0, min(g0 + exact, blocks)):
                found = ids[:, pl.ds(g * lanes, lanes)].astype(F32).astype(jnp.bfloat16)
                for j in range(top):
                    acc = acc + jnp.where(found[j:j + 1] == numbers, one, zero)
            total = total + jnp.sum(acc.astype(F32).T, axis=0, keepdims=True)
        cnt[0] = total.astype(jnp.int32)
        bias_in.wait()

    @pl.when(jnp.logical_not(is_root))
    def _():
        pl.semaphore_wait(barrier, 3)
        pl.semaphore_signal(ready, inc=1, device_id=(t, ROOT), device_id_type=MESH)
        bias_out.start()
        ids_in.wait()

    queue = list(range(AHEAD, nu))

    def more_tokens(freed):
        if queue and slot[queue[0]] == freed:
            x_in[queue.pop(0)].start()

    def send_counts():
        pl.semaphore_wait(barrier, ntok - 1)
        for copy in cnt_out:
            copy.start()

    def send_counts_soon():
        pl.when(jnp.logical_and(is_root, 2 * t >= ntok))(send_counts)

    def send_counts_late():
        pl.when(jnp.logical_and(is_root, 2 * t < ntok))(send_counts)

    def finish_counts():
        @pl.when(is_root)
        def _():
            cnt_all.wait()
            bias_back.wait_recv()
            total = cnt[0]
            for d in range(1, ntok):
                total = total + cnt[d]
            load = total.astype(F32)
            target = F32(ntok * rows * top)
            gap = target - F32(experts) * load
            sign = jnp.where(gap > 0, F32(1), jnp.where(gap < 0, F32(-1), F32(0)))
            bias = jnp.concatenate([bias_all[k] for k in range(4)], axis=1)
            for j in range(4):
                fin[j, 0] = load
                fin[j, 1] = bias + 0.001 * sign
            for copy in fin_out:
                copy.start()

    def close_counts():
        @pl.when(is_root)
        def _():
            fin_all.wait_send()

        @pl.when(jnp.logical_not(is_root))
        def _():
            fin_out[0].wait_recv()
            bias_out.wait_send()

        thin[...] = fin[3]

    def first(at, k):
        return pltpu.make_async_remote_copy(
            src_ref=part.at[1 - c, at], dst_ref=rx1.at[at],
            send_sem=s1, recv_sem=r1.at[k], device_id=(t, mate), device_id_type=MESH)

    def second(at, k):
        return pltpu.make_async_remote_copy(
            src_ref=tx2.at[at], dst_ref=rx2.at[at],
            send_sem=s2, recv_sem=r2.at[k], device_id=(t, peer), device_id_type=MESH)

    def raw(j):
        return pltpu.make_async_remote_copy(
            src_ref=tx2.at[0, :, within(j)], dst_ref=rx2.at[0, :, within(j)],
            send_sem=s2, recv_sem=r2.at[0], device_id=(t, peer), device_id_type=MESH)

    def across(j):
        return pltpu.make_async_remote_copy(
            src_ref=tx2.at[n, :, within(j)], dst_ref=rx2.at[n, :, within(j)],
            send_sem=s2, recv_sem=r2.at[0], device_id=(t, cross), device_id_type=MESH)

    chosen_out = pltpu.make_async_remote_copy(
        src_ref=tx3, dst_ref=rx3, send_sem=s3, recv_sem=r3, device_id=(t, peer), device_id_type=MESH)
    hand_on = pltpu.make_async_remote_copy(
        src_ref=rx3, dst_ref=rx3, send_sem=s3, recv_sem=r3, device_id=(t, mate), device_id_type=MESH)

    def arrival(i, runs, copy, blocks):
        for k, run in enumerate(runs):
            if run[0] == i:
                copy(pl.ds(0, sum(blocks(m) for m in run)), k).wait_recv()

    side = 256
    tiles = depth // side
    shares = [[(q, k) for q in (0, 1) for k in range(tiles)
               if (k < (tiles + 1 - i % 2) // 2) == (q == 0)] for i in range(nu)]
    line = [[(i, k) for i in range(nu) for p, k in shares[i] if p == q] for q in (0, 1)]
    where = [0, 0]

    def push(q):
        if where[q] < len(line[q]):
            k = line[q][where[q]][1]
            pltpu.matmul_push_rhs(wv[pl.ds(k * side, side), :], staging_register=where[q] % 2, mxu_index=q)

    def issue(i):
        x_in[i].wait()
        more_tokens(slot[i])
        left = [[k for p, k in shares[i] if p == q] for q in (0, 1)]
        for step in range(max(map(len, left))):
            for q in (0, 1):
                if step < len(left[q]):
                    k = left[q][step]
                    mark = where[q] % 2
                    where[q] += 1
                    push(q)
                    pltpu.matmul_acc_lhs(accs[acc_of[i]][q], xv[unit(i), pl.ds(k * side, side)], load_staged_rhs=mark)

    def product(j):
        if 0 < j < nu - 1:
            issue(j + 1)
        r = (pltpu.matmul_pop(accs[acc_of[j]][0]) + pltpu.matmul_pop(accs[acc_of[j]][1])).T
        for k in range(4):
            part[k % 2, units[j][2], pl.ds(k // 2 * own, own), within(j)] = r[k * own:(k + 1) * own]

    def pick(i):
        mine_ids = ids[:, cols(i)]
        low, high = mine_ids & 7, mine_ids >> 3
        picked = jnp.zeros(mine_ids.shape, F32)
        for k in range(experts // 8):
            block, line = divmod(8 * k, own)
            rows8 = part[block % 2, i, pl.ds(block // 2 * own + line, 8), :]
            row = jnp.take_along_axis(rows8, low, axis=0, mode="promise_in_bounds")
            picked = jnp.where(high == k, row, picked)
        for k in range(2):
            part[k, i, pl.ds(2 * own, top), :] = picked

    def to_mate(i):
        pick(i)
        first(i, mate_run[i]).start()

    def stage_a(j):
        product(j)
        if j == 0:
            @pl.when(is_root)
            def _():
                pl.semaphore_wait(ready, 3)
        start, width, i = units[j]
        if i == 0:
            tx2[0, :, within(j)] = encode(part[c, 0, theirs, within(j)]).astype(LINK)
            tx2[n, :, within(j)] = encode(part[1 - c, 0, theirs, within(j)]).astype(LINK)
            raw(j).start()
            across(j).start()
        else:
            to_mate(i)
        if j == 0:
            issue(1)
        if j == RAW_AT[-1] + 1:
            to_mate(0)

    bound = 2 * depth * TOKEN_BOUND * GATE_BOUND
    grain = TOP_CODE / math.asinh(bound)

    def encode(v):
        size = jnp.abs(v)
        code = jnp.log(size + jnp.sqrt(size * size + F32(1))) * F32(grain) + F32(0.5)
        return jnp.where(v < 0, -code, code).astype(jnp.int32)

    def decode(whole):
        grown = jnp.exp(whole.astype(F32) * F32(1 / grain))
        return F32(0.5) * grown - F32(0.5) / grown

    theirs = pl.ds(pl.multiple_of((1 - y) * own, own), own)
    ours = pl.ds(pl.multiple_of(y * own, own), own)
    picks = pl.ds(2 * own, top)

    def stage_b(i, core):
        arrival(i, mate_runs, first, lambda m: 1)
        if i > 0:
            tx2[i] = encode(part[c, i, theirs] + rx1[i, theirs]).astype(LINK)
            if core == 0 or i < n - HELD:
                second(i, peer_run[i]).start()
        chosen = encode(part[c, i, picks] + rx1[i, picks])
        if core == 1:
            tx3[:, cols(i)] = chosen.astype(LINK)
        if core == 1 and i == n - 1:
            chosen_out.start()
            for k in range(n - HELD, n):
                second(k, peer_run[k]).start()
        keep[:, cols(i)] = part[c, i, ours] + rx1[i, ours]
        mine[:, cols(i)] = decode(chosen)

    def weigh():
        chosen = 1.0 / (1.0 + jnp.exp(-(mine[...] + decode(rx3[...].astype(jnp.int32)))))
        wide[own:] = 2.5 * chosen / jnp.sum(chosen, axis=0, keepdims=True)

    def stage_c(i):
        arrival(i, peer_runs, second, lambda m: 2 if m == 0 else 1)
        logits = keep[:, cols(i)] + decode(rx2[i].astype(jnp.int32))
        if i == 0:
            logits = logits + decode(rx2[n].astype(jnp.int32))
        wide[0:own, cols(i)] = 1.0 / (1.0 + jnp.exp(-logits))

    w_all.wait()
    more_tokens(0)
    for q in (0, 1):
        push(q)
    issue(0)
    for kind, i in plan(n):
        if kind == "a":
            stage_a(i)
        else:
            pl.when(c == kind)(functools.partial(stage_b, i, kind))
        if (kind, i) == ("a", 1):
            send_counts_soon()
        if (kind, i) == ("a", n):
            send_counts_late()
    for i in range(n):
        if i == n - HELD:
            @pl.when(c == 1)
            def _():
                chosen_out.wait()
                hand_on.start()
            finish_counts()
        if i == n - 1:
            pl.when(c == 0)(hand_on.wait_recv)
            weigh()
            close_counts()
            first(pl.ds(0, n), 0).wait_send()
            second(pl.ds(0, n + 1), 0).wait_send()
            pl.when(c == 1)(hand_on.wait_send)
        stage_c(i)


def place(wide, thin, aff_hbm, wts_hbm, load_hbm, newb_hbm, sem):
    for k, (source, results) in enumerate(((wide, (aff_hbm, wts_hbm)), (thin, (load_hbm, newb_hbm)))):
        at = 0
        for result in results:
            pltpu.make_async_copy(source.at[pl.ds(at, result.shape[0])], result, sem.at[k]).start()
            at += result.shape[0]
    for k, source in enumerate((wide, thin)):
        pltpu.make_async_copy(source, source, sem.at[k]).wait()


def local(ntok, tokens, gate_weight, expert_ids, expert_bias):
    rows, depth = tokens.shape
    experts = gate_weight.shape[1]
    own = expert_bias.shape[0]
    top = expert_ids.shape[1]
    piece = 256
    widths = [piece] * (rows // piece)
    n = len(widths)
    dma = pltpu.SemaphoreType.DMA
    vm = pltpu.VMEM
    any_ = pl.BlockSpec(memory_space=pl.ANY)
    vmem = pl.BlockSpec(memory_space=pltpu.VMEM)
    shapes = ((own, rows), (top, rows), (1, 1, experts), (1, 1, experts))
    results = pl.pallas_call(
        functools.partial(kernel, ntok, widths),
        out_shape=(pltpu.VMEM((own + top, rows), F32), pltpu.VMEM((2, 1, experts), F32)),
        in_specs=[any_] * 4,
        out_specs=(vmem,) * 2,
        scratch_shapes=[
            vm((rows, depth), tokens.dtype), vm((depth, experts), gate_weight.dtype),
            vm((top, rows), jnp.int32),
            vm((4, 1, own), F32),
            vm((2, n, 2 * own + top, piece), F32), vm((n, 2 * own + top, piece), F32),
            vm((own, rows), F32), vm((top, rows), F32),
            vm((n + 1, own, piece), LINK), vm((n + 1, own, piece), LINK),
            vm((top, rows), LINK), vm((top, rows), LINK),
            vm((ntok, 1, experts), jnp.int32), vm((4, 2, 1, experts), F32),
            dma((2 + AHEAD,)), dma, dma((len(grouped(turns(n), MATE_RUNS)),)),
            dma, dma((len(grouped(turns(n), PEER_RUNS)),)), dma, dma, dma, dma, dma,
            pltpu.SemaphoreType.REGULAR,
        ],
        compiler_params=pltpu.CompilerParams(
            collective_id=0, has_side_effects=True, vmem_limit_bytes=60 * 1024 * 1024),
    )(tokens, gate_weight, expert_ids.T, expert_bias.reshape(1, own))
    aff, wts, load, newb = pl.pallas_call(
        place,
        out_shape=tuple(jax.ShapeDtypeStruct(shape, F32) for shape in shapes),
        in_specs=[vmem] * 2,
        out_specs=(pl.BlockSpec(memory_space=pltpu.HBM),) * 4,
        scratch_shapes=[dma((2,))],
    )(*(pltpu.with_memory_space_constraint(r, pltpu.VMEM) for r in results))
    return aff.T, wts.T, load.reshape(experts), newb.reshape(experts)


def solution(mesh):
    in_specs = (P("tok", "exp"), P("exp", None), P("tok", None), P("exp"))
    out_specs = (P("tok", "exp"), P("tok", None), P(), P())
    return jax.shard_map(functools.partial(local, mesh.shape["tok"]), mesh=mesh,
                         in_specs=in_specs, out_specs=out_specs, check_vma=False)
```
